32 devices in a mesh: dom: 16 (over z, x, core), rep: 2 (over y).
Axes of the slice: x: 2, y: 2, z: 4, core: 2. Of those that a mesh axis runs over, the one named last changes fastest.
Arguments:
- node_feats: bfloat16 [12288, 256], P(('dom', 'rep')), may hold values from -6 to 6
- node_ids: int32 [12288], replicated, may hold values from 0 to 16777215
- tile_row: int32 [16, 2, 16], replicated, may hold values from -1 to 95, as said below
- tile_col: int32 [16, 2, 16], replicated, may hold values from -1 to 95, as said below
- tile_count: int32 [16, 2, 16], replicated, may hold values from 1 to 128, as said below
- self_weight: bfloat16 [256, 512], replicated, may hold values from -0.375 to 0.375
- neigh_weight: bfloat16 [256, 512], replicated, may hold values from -3 to 3
- out_grad: bfloat16 [12288, 512], P(('dom', 'rep')), may hold values from -6 to 6
Outputs:
- hidden_out: bfloat16 [12288, 512], P(('dom', 'rep'))
- feat_grad: bfloat16 [12288, 256], P(('dom', 'rep'))
- self_grad: float32 [256, 512], replicated
- neigh_grad: float32 [256, 512], replicated
The draws below stay inside these ranges and needn't reach their ends.
Inputs may be any that keep to these rules, and one draw needn't show every extreme that they name: `tile_row`: entry [d, r, s] is -1 where the slot holds no tile, else a block row of dom group d: d * 6 plus 0 to 5. In every draw some pair (d, r) has all 16 of its slots filled. `tile_col`: -1 exactly where tile_row is -1; else one of the blocks of device (s, r): s * 6 + r * 3 plus 0 to 2. `tile_count`: read only where a tile is present.
All inputs are finite; a program needn't handle non-finite values.
Results may differ from the reference program's by a relative error of at most 0.01.
Values may be sent and summed in bfloat16 or wider, within the bound.
A program may use at most 64 MiB of HBM per device.

```python
import math
import jax
import jax.numpy as jnp
from jax import lax

TILE = 128
F_IN = 256
F_OUT = 512
BPD = 3
NODES = 12288
N_DOM = 16
N_REP = 2


def tile_pattern(key):
    folded = jax.random.fold_in(key, 4242)
    subkeys = jax.random.split(folded, 9)
    slot_shape = (N_DOM, N_REP, N_DOM)
    group_blocks = BPD * N_REP
    fill_rates = jax.random.randint(subkeys[0], (N_DOM, 1, 1), 2, 9)
    filled = jax.random.randint(subkeys[1], slot_shape, 0, 8) < fill_rates
    full_dom = jax.random.randint(subkeys[2], (), 0, N_DOM)
    full_rep = jax.random.randint(subkeys[3], (), 0, N_REP)
    forced = (jnp.arange(N_DOM)[:, None, None] == full_dom) & (jnp.arange(N_REP)[None, :, None] == full_rep)
    filled = filled | forced
    first_draw = jax.random.randint(subkeys[4], slot_shape, 0, group_blocks)
    second = jax.random.randint(subkeys[5], slot_shape, 0, group_blocks)
    row_order = jax.random.permutation(subkeys[6], group_blocks)
    local_row = row_order[jnp.minimum(first_draw, second)]
    row_block = jnp.arange(N_DOM)[:, None, None] * group_blocks + local_row
    col_block = jnp.arange(N_DOM)[None, None, :] * group_blocks + jnp.arange(N_REP)[None, :, None] * BPD + jax.random.randint(subkeys[7], slot_shape, 0, BPD)
    count_draws = jax.random.randint(subkeys[8], (2,) + slot_shape, 1, TILE + 1)
    counts = (count_draws[0] * count_draws[1] + TILE - 1) // TILE
    return (jnp.where(filled, row_block, -1).astype(jnp.int32), jnp.where(filled, col_block, -1).astype(jnp.int32), counts.astype(jnp.int32))


def draw_tile_row(key, part):
    return tile_pattern(key)[0]


def draw_tile_col(key, part):
    return tile_pattern(key)[1]


def draw_tile_count(key, part):
    return tile_pattern(key)[2]


def set_ends(result, key, low, top_value):
    extent = result.shape
    place = [jax.random.randint(jax.random.fold_in(key, axis), (), 0, extent[axis]) for axis in range(len(extent))]
    result = result.at[tuple(place)].set(low)
    longest = extent.index(max(extent))
    place[longest] = (place[longest] + 1) % extent[longest]
    return result.at[tuple(place)].set(top_value)


def levels(rng, extent, shards, least, top_value):
    factor_of, own = 1.0, jax.random.fold_in(rng, 6)
    for axis_at, blocks in shards:
        draws = jnp.exp(jax.random.uniform(jax.random.fold_in(own, axis_at), (blocks,), jnp.float32, least / len(shards), top_value / len(shards)))
        factor_of = factor_of * jnp.repeat(draws, extent[axis_at] // blocks).reshape([-1 if axis == axis_at else 1 for axis in range(len(extent))])
    return factor_of


def centred(own_key, extent, deviation, limit, cuts=(), kind=jnp.bfloat16):
    result = jax.random.normal(own_key, extent, jnp.float32) * deviation
    if len(cuts) > 0:
        result = levels(own_key, extent, cuts, -0.22, 0.18) * result
    return jnp.clip(result, min=-limit, max=limit).astype(kind)


def setup_inputs(seed: int = 0) -> dict:
    keys = jax.random.split(jax.random.key(seed), 9)
    return {
        "node_feats": centred(keys[0], (NODES, F_IN), 1.0, 6.0, ((0, 32),)),
        "node_ids": set_ends(jax.random.randint(keys[1], (NODES,), 0, 16777216 // ((NODES + 65520) // 65521)), jax.random.fold_in(keys[1], 1), 0, (16777216 // ((NODES + 65520) // 65521)) - 1).astype(jnp.int32),
        "tile_row": draw_tile_row(jax.random.fold_in(keys[8], 71), 0),
        "tile_col": draw_tile_col(jax.random.fold_in(keys[8], 71), 0),
        "tile_count": draw_tile_count(jax.random.fold_in(keys[8], 71), 0),
        "self_weight": centred(keys[5], (F_IN, F_OUT), F_IN ** -0.5, 0.375),
        "neigh_weight": centred(keys[6], (F_IN, F_OUT), (max(F_IN // 64, 1)) ** -0.5, 3.0),
        "out_grad": centred(keys[7], (NODES, F_OUT), 1.0, 6.0, ((0, 32),)),
    }


def edge_masks(row_ids, col_ids, limits):
    left_ids = (row_ids % 4093)[:, :, None]
    right_ids = (col_ids % 4091)[:, None, :]
    hashed = (left_ids * right_ids + left_ids + 3 * right_ids) % 4099 % TILE
    return (hashed < limits[:, None, None]).astype(jnp.float32)

def slot_masks(id_blocks, rows_in, cols_in, limits_in):
    present = rows_in >= 0
    row_block = jnp.where(present, rows_in, 0)
    col_block = jnp.where(present, cols_in, 0)
    limits = jnp.where(present, limits_in, 0)
    tile_masks = edge_masks(id_blocks[row_block], id_blocks[col_block], limits)
    return (tile_masks, row_block, col_block, present)

def reference(node_feats, node_ids, tile_row, tile_col, tile_count, self_weight, neigh_weight, out_grad):
    node_count, width_in = node_feats.shape
    block_count = node_count // TILE
    group_blocks = block_count // N_DOM
    id_blocks = node_ids.reshape(block_count, TILE)
    feat_blocks = node_feats.astype(jnp.float32).reshape(block_count, TILE, width_in)

    def forward_group(group_index):
        tile_masks, row_block, col_block, present = slot_masks(id_blocks, tile_row[group_index].reshape(-1), tile_col[group_index].reshape(-1), tile_count[group_index].reshape(-1))
        products = jnp.einsum('sij,sjf->sif', tile_masks, feat_blocks[col_block])
        offset = row_block - group_index * group_blocks
        select = ((offset[:, None] == jnp.arange(group_blocks)[None, :]) & present[:, None]).astype(jnp.float32)
        partial_value = jnp.einsum('rsb,rsif->rbif', select.reshape(N_REP, N_DOM, group_blocks), products.reshape(N_REP, N_DOM, TILE, width_in))
        rounded = lax.optimization_barrier(partial_value.astype(jnp.bfloat16))
        return lax.optimization_barrier(jnp.sum(rounded.astype(jnp.float32), axis=0))
    summed = lax.map(forward_group, jnp.arange(N_DOM)).reshape(node_count, width_in)
    flat_rows = tile_row.reshape(-1)
    flat_limits = tile_count.reshape(-1)
    present_all = flat_rows >= 0
    degree = jnp.zeros((block_count,), jnp.float32).at[jnp.where(present_all, flat_rows, 0)].add(jnp.where(present_all, flat_limits, 0).astype(jnp.float32))
    divisor = jnp.repeat(jnp.maximum(degree, 1.0), TILE)[:, None]
    mean_feats = (summed / divisor).astype(jnp.bfloat16)
    preact = jnp.dot(node_feats, self_weight, preferred_element_type=jnp.float32) + jnp.dot(mean_feats, neigh_weight, preferred_element_type=jnp.float32)
    hidden_out = jax.nn.silu(preact).astype(jnp.bfloat16)
    logistic = jax.nn.sigmoid(preact)
    pre_grad = (out_grad.astype(jnp.float32) * logistic * (1.0 + preact * (1.0 - logistic))).astype(jnp.bfloat16)
    grad_scale = 1.0 / math.sqrt(node_count)
    self_grad = jnp.dot(node_feats.T, pre_grad, preferred_element_type=jnp.float32) * grad_scale
    neigh_grad = jnp.dot(mean_feats.T, pre_grad, preferred_element_type=jnp.float32) * grad_scale
    mean_grad = jnp.dot(pre_grad, neigh_weight.T, preferred_element_type=jnp.float32)
    spread = (mean_grad / divisor).astype(jnp.bfloat16)
    spread_blocks = spread.astype(jnp.float32).reshape(block_count, TILE, width_in)

    def backward_group(running, group_index):
        tile_masks, row_block, col_block, present = slot_masks(id_blocks, tile_row[group_index].reshape(-1), tile_col[group_index].reshape(-1), tile_count[group_index].reshape(-1))
        products = jnp.einsum('sij,sif->sjf', tile_masks, spread_blocks[row_block])
        return (running.at[col_block].add(products), None)
    transposed, _ = lax.scan(backward_group, jnp.zeros((block_count, TILE, width_in), jnp.float32), jnp.arange(N_DOM))
    feat_grad = (jnp.dot(pre_grad, self_weight.T, preferred_element_type=jnp.float32) + transposed.reshape(node_count, width_in)).astype(jnp.bfloat16)
    return (hidden_out, feat_grad, self_grad, neigh_grad)
```

```python
import functools
import math

import jax
import jax.numpy as jnp
from jax import lax
from jax.experimental import pallas as pl
from jax.experimental.pallas import tpu as pltpu
from jax.sharding import PartitionSpec as P

TILE = 128
LANES = 128
HASH = 4099.0

MESH = pl.DeviceIdType.MESH
OVER_ROWS = (((0,), (0,)), ((), ()))
OVER_COLS = (((1,), (1,)), ((), ()))
BF16 = jnp.bfloat16
F32 = jnp.float32


def modulo(value, base):
    quotient = jnp.floor(value * ((1.0 - 2.0**-20) / base))
    left = value - quotient * base
    return jnp.where(left >= base, left - base, left)


def across(row):
    return jnp.broadcast_to(row, (TILE, TILE)).T


def bucket(hashed):
    left = modulo(hashed, HASH)
    return left - jnp.floor(left * (1.0 / TILE)) * TILE


class Plan:
    def __init__(self, dom_total, rep_total, rows, width_in, width_out):
        self.line = math.gcd(dom_total, 4)
        self.plane = dom_total // self.line
        self.cores = math.gcd(self.plane, 2)
        self.cols = self.plane // self.cores
        self.reps = rep_total
        self.doms = dom_total
        self.own = rows // TILE
        self.group = self.own * rep_total
        self.halves = width_in // LANES
        self.width_in, self.width_out = width_in, width_out
        self.ring = self.cols * rep_total
        self.strip = 2 * width_in // (self.cores * self.ring * self.line)
        self.split = self.strip % 16 == 0
        self.ahead = self.line * self.group * self.plane * TILE * TILE * 2 <= 2**23


def fused(plan, scale, *refs):
    refs = list(refs)

    def take(count):
        out, refs[:count] = refs[:count], []
        return out

    line, plane, reps, own, group, halves = (
        plan.line, plan.plane, plan.reps, plan.own, plan.group, plan.halves,
    )
    tile_row, tile_col, tile_count, ids, x, cot, w_self, w_neigh = take(8)
    hidden, feat_grad, grads = take(3)
    left_ids, right_ids, wide, tall = take(4)
    held, chosen, picked, total, partial, landed, mean, preact, back = take(9)
    spread = take(halves)
    picked_back, chosen_back, sums_out, sums_in = take(4)
    if plan.split:
        terms, first_in, first, second_in, second, third_in, final = take(7)
    line_sems, pick_sems, rep_sems, spread_sems, pick_back_sems, sum_sems = take(6)
    if plan.split:
        core_sems, ring_sems, far_sems, far_back_sems, ring_back_sems, core_back_sems = take(6)

    dom, rep = lax.axis_index("dom"), lax.axis_index("rep")
    z, p = dom // plane, lax.rem(dom, plane)

    def device(zz, pp, rr):
        return (zz * plane + pp, rr)

    def remote(src, dst, sems, index, target):
        return pltpu.make_async_remote_copy(
            src_ref=src,
            dst_ref=dst,
            send_sem=sems.at[(0,) + index],
            recv_sem=sems.at[(1,) + index],
            device_id=target,
            device_id_type=MESH,
        )

    line_peers = [lax.rem(z + k, line) for k in range(1, line)]
    plane_peers = [lax.rem(p + k, plane) for k in range(1, plane)]
    rep_peers = [lax.rem(rep + k, reps) for k in range(1, reps)]
    col, core = p // plan.cores, lax.rem(p, plan.cores)

    everyone = [device(other, p, rep) for other in line_peers]
    everyone += [device(z, other, rep) for other in plane_peers]
    for k in range(plan.cols):
        other = lax.rem(col + k, plan.cols) * plan.cores + core
        everyone += [device(z, other, peer) for peer in rep_peers]
    barrier = pltpu.get_barrier_semaphore()
    for peer in everyone:
        pl.semaphore_signal(barrier, inc=1, device_id=peer, device_id_type=MESH)

    node = ids[...].astype(F32)
    left_ids[...] = modulo(node, 4093.0)
    right_ids[...] = modulo(node, 4091.0)

    home = line - 1
    levels = [[(above, k) for above in range(2)] for k in range(1, line)]

    def slot_of(above, k):
        return line - 1 - k if above else k - 1

    def spot(above, k):
        return z + k if above else z - k

    def exists(above, k):
        return z < line - k if above else z >= k

    def half(h):
        return slice(h * LANES, (h + 1) * LANES)

    def passes_on(above):
        return z >= 1 if above else z < line - 1

    def line_copy(h, above, k):
        slot = slot_of(above, k + 1)
        src = held.at[h, slot_of(above, k)] if k else x.at[:, :, half(h)]
        return remote(
            src, held.at[h, slot], line_sems, (above, h, k), device(z + 1 - 2 * above, p, rep)
        )

    pl.semaphore_wait(barrier, len(everyone))

    def choose(h, slot, source, blocks):
        first_own = ((source * plane + p) * reps + rep) * own

        def block_for(d):
            offset = tile_col[d, rep, source * plane + p] - first_own
            value = blocks[0]
            for b in range(1, own):
                value = lax.select(offset == b, blocks[b], value)
            return value

        for k, peer in enumerate(plane_peers):
            chosen[h, slot, k] = block_for(z * plane + peer)
            pick_copy(h, slot, k).start()
        picked[h, slot, plane - 1] = block_for(dom)

    def pick_copy(h, slot, k):
        return remote(
            chosen.at[h, slot, k], picked.at[h, slot, k], pick_sems, (h, slot, k),
            device(z, plane_peers[k], rep),
        )

    for h in range(halves):
        for above in range(2):
            @pl.when(passes_on(above))
            def _():
                line_copy(h, above, 0).start()
    for h in range(halves):
        choose(h, home, z, [x[b, :, half(h)] for b in range(own)])

    group_first = dom * group
    own_first = (dom * reps + rep) * own

    def each(count, body):
        if plan.ahead:
            for i in range(count):
                body(i)
        else:
            lax.fori_loop(0, count, lambda i, c: (body(i), c)[1], 0)

    def span(i):
        return pl.ds(pl.multiple_of(i * TILE, TILE), TILE)

    def build_wide(source, slot):
        def tile(other):
            s = source * plane + lax.rem(p + 2 * plane - 1 - other, plane)
            row, column = tile_row[dom, rep, s], tile_col[dom, rep, s]
            present = row >= 0
            limit = jnp.where(present, tile_count[dom, rep, s], 0)
            row_block = jnp.where(present, row, 0)
            left = across(left_ids[pl.ds(row_block, 1), :])
            right = right_ids[pl.ds(jnp.where(present, column, 0), 1), :]
            bits = bucket(left * (right + 1.0) + 3.0 * right)

            def place(b):
                here = jnp.where(row_block - group_first == b, limit, 0).astype(F32)
                wide[slot, span(b), span(other)] = jnp.where(bits < here, 1.0, 0.0).astype(BF16)

            each(group, place)

        each(plane, tile)

    def build_tall(target):
        s = target * plane + p
        first_own = (s * reps + rep) * own

        def tile(other):
            d = z * plane + lax.rem(p + 2 * plane - 1 - other, plane)
            row, column = tile_row[d, rep, s], tile_col[d, rep, s]
            present = row >= 0
            limit = jnp.where(present, tile_count[d, rep, s], 0)
            left = left_ids[pl.ds(jnp.where(present, row, 0), 1), :]
            right = across(right_ids[pl.ds(jnp.where(present, column, 0), 1), :])
            bits = bucket(left * (right + 1.0) + 3.0 * right)
            for b in range(own):
                here = jnp.where(column - first_own == b, limit, 0).astype(F32)
                tall[target, span(b), span(other)] = jnp.where(bits < here, 1.0, 0.0).astype(BF16)

        each(plane, tile)

    if plan.ahead:
        lax.fori_loop(0, line, lambda i, c: (build_wide(i, i), c)[1], 0)
    lax.fori_loop(0, line, lambda i, c: (build_tall(i), c)[1], 0)

    def count_degrees(s, carry):
        for other in range(reps):
            row, limit = tile_row[dom, other, s], tile_count[dom, other, s]
            carry = tuple(
                value + jnp.where(row == own_first + b, limit, 0) for b, value in enumerate(carry)
            )
        return carry

    degrees = lax.fori_loop(0, plan.doms, count_degrees, (jnp.int32(0),) * own)
    inverse = [
        1.0 / jnp.maximum(jnp.full((8, LANES), degree, jnp.int32).astype(F32), 1.0)[:1]
        for degree in degrees
    ]

    flat_x = x[...].reshape(own * TILE, plan.width_in)
    preact[...] = jnp.dot(flat_x, w_self[...], preferred_element_type=F32)

    def consume(h, slot, source, start):
        for k in range(plane - 1):
            pick_copy(h, slot, k).wait_recv()
        features = picked[h, slot].reshape(plane * TILE, LANES)
        if plan.ahead:
            value = jnp.dot(wide[source], features, preferred_element_type=F32)
            total[h] = value if start else total[h] + value
            return
        build_wide(source, 0)

        def rows(b):
            value = jnp.dot(wide[0, span(b)], features, preferred_element_type=F32)
            total[h, span(b)] = value if start else total[h, span(b)] + value

        each(group, rows)

    def arrive(h, above, k):
        line_copy(h, above, k - 1).wait_recv()

        if k < line - 1:
            @pl.when(passes_on(above))
            def _():
                line_copy(h, above, k).start()

        slot = slot_of(above, k)
        choose(h, slot, spot(above, k), [held[h, slot, b] for b in range(own)])

    def rep_copy(h, peer, slot):
        return remote(
            partial.at[h, peer], landed.at[h, slot], rep_sems, (h, slot), device(z, p, peer)
        )

    def send_partials(h):
        partial[h] = total[h].astype(BF16).reshape(reps, own, TILE, LANES)
        for k, peer in enumerate(rep_peers):
            rep_copy(h, peer, k).start()

    def consume_level(h, k):
        if k == 0:
            consume(h, home, z, True)
            return
        for above, k in levels[k - 1]:
            @pl.when(exists(above, k))
            def _():
                consume(h, slot_of(above, k), spot(above, k), False)

    for k in range(1, line):
        for h in range(halves):
            for above in range(2):
                @pl.when(exists(above, k))
                def _():
                    arrive(h, above, k)
        for h in range(halves):
            consume_level(h, k - 1)
    for h in range(halves):
        consume_level(h, line - 1)
        send_partials(h)

    for h in range(halves):
        for k, peer in enumerate(rep_peers):
            rep_copy(h, peer, k).wait_recv()
        for b in range(own):
            summed = partial[h, rep, b].astype(F32)
            for k in range(reps - 1):
                summed = summed + landed[h, k, b].astype(F32)
            mean[b * TILE : (b + 1) * TILE, half(h)] = (summed * inverse[b]).astype(BF16)
        preact[...] += jnp.dot(
            mean[:, half(h)], w_neigh[half(h), :], preferred_element_type=F32
        )
    value = preact[...]
    logistic = jax.nn.sigmoid(value)
    grad = (cot[...].astype(F32) * logistic * (1.0 + value * (1.0 - logistic))).astype(BF16)
    hidden[...] = (value * logistic).astype(BF16)

    def spread_copy(h, peer, slot):
        return remote(
            spread[h].at[rep], spread[h].at[rep], spread_sems, (h, slot), device(z, p, peer)
        )

    def spread_arrived(h, k):
        source = lax.rem(rep + reps - k - 1, reps)
        return remote(
            spread[h].at[source], spread[h].at[source], spread_sems, (h, k), device(z, p, source)
        )

    for h in range(halves):
        product = lax.dot_general(grad, w_neigh[half(h), :], OVER_COLS, preferred_element_type=F32)
        for b in range(own):
            spread[h][rep, b] = (product[b * TILE : (b + 1) * TILE] * inverse[b]).astype(BF16)
        for k, peer in enumerate(rep_peers):
            spread_copy(h, peer, k).start()

    both = (x[...].reshape(own * TILE, plan.width_in), mean[...])
    ring_at = col * reps + rep
    ring_peers = []
    for k in range(1, plan.ring):
        other = lax.rem(ring_at + k, plan.ring)
        ring_peers.append(
            (other, device(z, (other // reps) * plan.cores + core, lax.rem(other, reps)))
        )
    core_peers = []
    for k in range(1, plan.cores):
        other = lax.rem(core + k, plan.cores)
        core_peers.append((other, device(z, col * plan.cores + other, rep)))
    far_peers = [(other, device(other, p, rep)) for other in line_peers]

    stages = []
    if plan.split:
        for i, rows in enumerate(both):
            product = lax.dot_general(rows, grad, OVER_ROWS, preferred_element_type=F32)
            piece = product.astype(BF16).reshape(-1, plan.strip, plan.width_out)
            count = piece.shape[0]
            terms[i * count : (i + 1) * count] = piece
        per_core = plan.ring * plan.line

        def core_copies():
            return [
                remote(
                    terms.at[pl.ds(other * per_core, per_core)], first_in.at[k], core_sems, (k,), to
                )
                for k, (other, to) in enumerate(core_peers)
            ]

        def ring_copies():
            return [
                remote(
                    first.at[pl.ds(other * line, line)], second_in.at[k], ring_sems, (k,), to
                )
                for k, (other, to) in enumerate(ring_peers)
            ]

        def far_copies():
            return [
                remote(second.at[other], third_in.at[k], far_sems, (k,), to)
                for k, (other, to) in enumerate(far_peers)
            ]

        def place(c, q, zz):
            return (c * plan.ring + q) * line + zz

        def far_back_copies():
            return [
                remote(final, grads.at[place(core, ring_at, z)], far_back_sems, (k,), to)
                for k, (_, to) in enumerate(far_peers)
            ]

        def ring_back_copies():
            block = grads.at[pl.ds(place(core, ring_at, 0), line)]
            return [
                remote(block, block, ring_back_sems, (k,), to)
                for k, (_, to) in enumerate(ring_peers)
            ]

        def core_back_copies():
            block = grads.at[pl.ds(place(core, 0, 0), per_core)]
            return [
                remote(block, block, core_back_sems, (k,), to)
                for k, (_, to) in enumerate(core_peers)
            ]

        def start(copies):
            for copy in copies:
                copy.start()

        def arrived(copies):
            for copy in copies:
                copy.wait_recv()

        def stage_core():
            arrived(core_copies())
            value = terms[pl.ds(core * per_core, per_core)].astype(F32)
            for k in range(len(core_peers)):
                value = value + first_in[k].astype(F32)
            first[...] = value.astype(BF16)
            start(ring_copies())

        def stage_ring():
            arrived(ring_copies())
            value = first[pl.ds(ring_at * line, line)].astype(F32)
            for k in range(len(ring_peers)):
                value = value + second_in[k].astype(F32)
            second[...] = value.astype(BF16)
            start(far_copies())

        def stage_far():
            arrived(far_copies())
            value = second[z].astype(F32)
            for k in range(len(far_peers)):
                value = value + third_in[k].astype(F32)
            value = (value * scale).astype(BF16)
            final[...] = value
            grads[place(core, ring_at, z)] = value
            start(far_back_copies())

        def stage_ring_back():
            arrived(far_back_copies())
            start(ring_back_copies())

        def stage_core_back():
            arrived(ring_back_copies())
            start(core_back_copies())

        start(core_copies())
        stages = [stage_core, stage_ring, stage_far, stage_ring_back, stage_core_back]
    else:
        for i, rows in enumerate(both):
            grads[i] = lax.dot_general(rows, grad, OVER_ROWS, preferred_element_type=F32)

    def next_stage():
        if stages:
            stages.pop(0)()

    back[...] = lax.dot_general(grad, w_self[...], OVER_COLS, preferred_element_type=F32)

    def pick_back_copy(h, slot, k):
        return remote(
            chosen_back.at[h, slot, k], picked_back.at[h, slot, k], pick_back_sems, (h, slot, k),
            device(z, plane_peers[k], rep),
        )

    def choose_back(h, slot, target):
        def block_for(peer):
            row = tile_row[dom, rep, target * plane + peer]
            offset = jnp.minimum(jnp.maximum(row - group_first, 0), group - 1)
            return spread[h][offset // own, lax.rem(offset, own)]

        for k, peer in enumerate(plane_peers):
            chosen_back[h, slot, k] = block_for(peer)
            pick_back_copy(h, slot, k).start()
        picked_back[h, slot, plane - 1] = block_for(p)

    for h in range(halves):
        for k in range(reps - 1):
            spread_arrived(h, k).wait_recv()
        for level in reversed(levels):
            for above, k in level:
                @pl.when(exists(above, k))
                def _():
                    choose_back(h, slot_of(above, k), spot(above, k))
        choose_back(h, home, z)
    next_stage()

    def sum_copy(h, above, k):
        slot = slot_of(above, k)
        nearer = slot_of(above, k - 1) if k > 1 else home
        return remote(
            sums_out.at[h, slot], sums_in.at[above, h, nearer], sum_sems, (above, h, k - 1),
            device(z + 2 * above - 1, p, rep),
        )

    def contribution(h, slot, target):
        for k in range(plane - 1):
            pick_back_copy(h, slot, k).wait_recv()
        return jnp.dot(
            tall[target],
            picked_back[h, slot].reshape(plane * TILE, LANES),
            preferred_element_type=F32,
        )

    def pass_sums(h, above, k):
        slot = slot_of(above, k)
        value = contribution(h, slot, spot(above, k))
        sums_out[h, slot] = value.astype(BF16)
        if k < line - 1:
            @pl.when(passes_on(above))
            def _():
                sum_copy(h, above, k + 1).wait_recv()
                sums_out[h, slot] = (
                    sums_out[h, slot].astype(F32) + sums_in[above, h, slot].astype(F32)
                ).astype(BF16)

        sum_copy(h, above, k).start()

    for level in reversed(levels):
        for above, k in level:
            @pl.when(exists(above, k))
            def _():
                for h in range(halves):
                    pass_sums(h, above, k)
        next_stage()
    for h in range(halves):
        back[:, half(h)] += contribution(h, home, z)
        for above in range(2 if line > 1 else 0):
            @pl.when(passes_on(above))
            def _():
                sum_copy(h, above, 1).wait_recv()
                back[:, half(h)] += sums_in[above, h, home].astype(F32)
        feat_grad[:, half(h)] = back[:, half(h)].astype(BF16)
    while stages:
        next_stage()
    if plan.split:
        arrived(core_back_copies())

    for h in range(halves):
        for above in range(2):
            @pl.when(passes_on(above))
            def _():
                line_copy(h, above, 0).wait_send()
            for k in range(1, line):
                if k < line - 1:
                    @pl.when(jnp.logical_and(exists(above, k), passes_on(above)))
                    def _():
                        line_copy(h, above, k).wait_send()

                @pl.when(exists(above, k))
                def _():
                    sum_copy(h, above, k).wait_send()
        for slot in range(line):
            for k in range(plane - 1):
                pick_copy(h, slot, k).wait_send()
                pick_back_copy(h, slot, k).wait_send()
        for k, peer in enumerate(rep_peers):
            rep_copy(h, peer, k).wait_send()
            spread_copy(h, peer, k).wait_send()
    if plan.split:
        for copies in (
            core_copies(), ring_copies(), far_copies(),
            far_back_copies(), ring_back_copies(), core_back_copies(),
        ):
            for copy in copies:
                copy.wait_send()


def dma(*shape):
    return pltpu.SemaphoreType.DMA(tuple(max(size, 1) for size in (2,) + shape))


def shards(
    node_feats, node_ids, tile_row, tile_col, tile_count, self_weight, neigh_weight, out_grad
):
    rows, width_in = node_feats.shape
    width_out = self_weight.shape[1]
    plan = Plan(lax.axis_size("dom"), lax.axis_size("rep"), rows, width_in, width_out)
    line, plane, reps, own, halves = plan.line, plan.plane, plan.reps, plan.own, plan.halves
    scale = 1.0 / math.sqrt(rows * plan.doms * reps)
    id_rows = node_ids.shape[0] // TILE

    def buffer(*shape, dtype=BF16):
        return pltpu.VMEM(tuple(max(size, 1) for size in shape), dtype)

    tile = (TILE, LANES)
    scratch = [
        buffer(id_rows, TILE, dtype=F32),
        buffer(id_rows, TILE, dtype=F32),
        buffer(line if plan.ahead else 1, plan.group * TILE, plane * TILE),
        buffer(line, own * TILE, plane * TILE),
        buffer(halves, line, own, *tile),
        buffer(halves, line, plane, *tile),
        buffer(halves, line, plane, *tile),
        buffer(halves, plan.group * TILE, LANES, dtype=F32),
        buffer(halves, reps, own, *tile),
        buffer(halves, reps - 1, own, *tile),
        buffer(rows, width_in),
        buffer(rows, width_out, dtype=F32),
        buffer(rows, width_in, dtype=F32),
        *[buffer(reps, own, *tile) for _ in range(halves)],
        buffer(halves, line, plane, *tile),
        buffer(halves, line, plane, *tile),
        buffer(halves, line, own * TILE, LANES),
        buffer(2, halves, line, own * TILE, LANES),
    ]
    strip = (plan.strip, width_out)
    per_core = plan.ring * line
    if plan.split:
        scratch += [
            buffer(plan.cores * per_core, *strip),
            buffer(plan.cores - 1, per_core, *strip),
            buffer(per_core, *strip),
            buffer(plan.ring - 1, line, *strip),
            buffer(line, *strip),
            buffer(line - 1, *strip),
            buffer(*strip),
        ]
    scratch += [
        dma(2, halves, line),
        dma(halves, line, plane),
        dma(halves, reps - 1),
        dma(halves, reps - 1),
        dma(halves, line, plane),
        dma(2, halves, line),
    ]
    if plan.split:
        scratch += [
            dma(plan.cores - 1), dma(plan.ring - 1), dma(line - 1),
            dma(line - 1), dma(plan.ring - 1), dma(plan.cores - 1),
        ]
        grads_shape = jax.ShapeDtypeStruct((plan.cores * per_core, *strip), BF16)
    else:
        grads_shape = jax.ShapeDtypeStruct((2, width_in, width_out), F32)
    vmem, smem = pl.BlockSpec(memory_space=pltpu.VMEM), pl.BlockSpec(memory_space=pltpu.SMEM)
    hidden_out, feat_grad, grads = pl.pallas_call(
        functools.partial(fused, plan, scale),
        out_shape=(
            jax.ShapeDtypeStruct((rows, width_out), BF16),
            jax.ShapeDtypeStruct((rows, width_in), BF16),
            grads_shape,
        ),
        in_specs=[smem] * 3 + [vmem] * 5,
        out_specs=(vmem,) * 3,
        scratch_shapes=scratch,
        compiler_params=pltpu.CompilerParams(collective_id=1, has_side_effects=True),
    )(
        tile_row,
        tile_col,
        tile_count,
        node_ids.reshape(id_rows, TILE),
        node_feats.reshape(own, TILE, width_in),
        out_grad,
        self_weight,
        neigh_weight,
    )
    if plan.split:
        grads = grads.reshape(2, width_in, width_out).astype(F32)
    else:
        grads = lax.psum(grads, ("dom", "rep")) * scale
    return hidden_out, feat_grad, grads[0], grads[1]


def solution(mesh):
    placed = (P(("dom", "rep"), None), P(), P(), P(), P(), P(), P(), P(("dom", "rep"), None))
    return jax.shard_map(
        shards,
        mesh=mesh,
        in_specs=placed,
        out_specs=(P(("dom", "rep"), None), P(("dom", "rep"), None), P(), P()),
        check_vma=False,
    )
```

```python
import functools
import math

import jax
import jax.numpy as jnp
from jax import lax
from jax.experimental import pallas as pl
from jax.experimental.pallas import tpu as pltpu
from jax.sharding import PartitionSpec as P

TILE = 128
LANES = 128
HASH = 4099.0

MESH = pl.DeviceIdType.MESH
OVER_ROWS = (((0,), (0,)), ((), ()))
OVER_COLS = (((1,), (1,)), ((), ()))
BF16 = jnp.bfloat16
F32 = jnp.float32


def modulo(value, base):
    quotient = jnp.floor(value * ((1.0 - 2.0**-20) / base))
    left = value - quotient * base
    return jnp.where(left >= base, left - base, left)


def across(row):
    return jnp.broadcast_to(row, (TILE, TILE)).T


def bucket(hashed):
    left = modulo(hashed, HASH)
    return left - jnp.floor(left * (1.0 / TILE)) * TILE


class Plan:
    def __init__(self, dom_total, rep_total, rows, width_in, width_out):
        self.line = math.gcd(dom_total, 4)
        self.plane = dom_total // self.line
        self.cores = math.gcd(self.plane, 2)
        self.cols = self.plane // self.cores
        self.reps = rep_total
        self.doms = dom_total
        self.own = rows // TILE
        self.group = self.own * rep_total
        self.halves = width_in // LANES
        self.width_in, self.width_out = width_in, width_out
        self.ring = self.cols * rep_total
        self.strip = 2 * width_in // (self.cores * self.ring * self.line)
        self.split = self.strip % 16 == 0 and self.cores == 2
        self.ahead = self.line * self.group * self.plane * TILE * TILE * 2 <= 2**23


def fused(plan, scale, *refs):
    refs = list(refs)

    def take(count):
        out, refs[:count] = refs[:count], []
        return out

    line, plane, reps, own, group, halves = (
        plan.line, plan.plane, plan.reps, plan.own, plan.group, plan.halves,
    )
    given = take(8)
    hidden, feat_grad, grads = take(3)
    inputs = take(8)
    tile_row, tile_col, tile_count, ids, x, cot, w_self, w_neigh = inputs
    left_ids, right_ids, wide, tall = take(4)
    held, chosen, picked, total, partial, landed, mean, preact, back = take(9)
    spread = take(halves)
    picked_back, chosen_back, sums_out, sums_in = take(4)
    if plan.split:
        terms, first_in, first, second_in, second, third_in, final = take(7)
    (load_sems,) = take(1)
    line_sems, pick_sems, rep_sems, spread_sems, pick_back_sems, sum_sems = take(6)
    if plan.split:
        core_sems, far_sems, ring_sems, far_back_sems, ring_back_sems, core_back_sems = take(6)

    dom, rep = lax.axis_index("dom"), lax.axis_index("rep")
    z, p = dom // plane, lax.rem(dom, plane)

    def device(zz, pp, rr):
        return (zz * plane + pp, rr)

    def remote(src, dst, sems, index, target):
        return pltpu.make_async_remote_copy(
            src_ref=src,
            dst_ref=dst,
            send_sem=sems.at[(0,) + index],
            recv_sem=sems.at[(1,) + index],
            device_id=target,
            device_id_type=MESH,
        )

    line_peers = [lax.rem(z + k, line) for k in range(1, line)]
    plane_peers = [lax.rem(p + k, plane) for k in range(1, plane)]
    rep_peers = [lax.rem(rep + k, reps) for k in range(1, reps)]
    col, core = p // plan.cores, lax.rem(p, plan.cores)

    everyone = [device(other, p, rep) for other in line_peers]
    everyone += [device(z, other, rep) for other in plane_peers]
    for k in range(plan.cols):
        other = lax.rem(col + k, plan.cols) * plan.cores + core
        everyone += [device(z, other, peer) for peer in rep_peers]
    loads = [
        pltpu.make_async_copy(src, dst, load_sems.at[i])
        for i, (src, dst) in enumerate(zip(given, inputs))
    ]
    for i in (4, 1, 3, 0, 2, 6, 7, 5):
        loads[i].start()
    barrier = pltpu.get_barrier_semaphore()
    for peer in everyone:
        pl.semaphore_signal(barrier, inc=1, device_id=peer, device_id_type=MESH)

    for i in (0, 1, 2, 3, 4):
        loads[i].wait()
    node = ids[...].astype(F32)
    left_ids[...] = modulo(node, 4093.0)
    right_ids[...] = modulo(node, 4091.0)

    home = line - 1
    levels = [[(above, k) for above in range(2)] for k in range(1, line)]

    def slot_of(above, k):
        return line - 1 - k if above else k - 1

    def spot(above, k):
        return z + k if above else z - k

    def exists(above, k):
        return z < line - k if above else z >= k

    def half(h):
        return slice(h * LANES, (h + 1) * LANES)

    def passes_on(above):
        return z >= 1 if above else z < line - 1

    def line_copy(h, above, k):
        slot = slot_of(above, k + 1)
        src = held.at[h, slot_of(above, k)] if k else x.at[:, :, half(h)]
        return remote(
            src, held.at[h, slot], line_sems, (above, h, k), device(z + 1 - 2 * above, p, rep)
        )

    pl.semaphore_wait(barrier, len(everyone))

    def choose(h, slot, source, blocks):
        first_own = ((source * plane + p) * reps + rep) * own

        def block_for(d):
            offset = tile_col[d, rep, source * plane + p] - first_own
            value = blocks[0]
            for b in range(1, own):
                value = lax.select(offset == b, blocks[b], value)
            return value

        for k, peer in enumerate(plane_peers):
            chosen[h, slot, k] = block_for(z * plane + peer)
            pick_copy(h, slot, k).start()
        picked[h, slot, plane - 1] = block_for(dom)

    def pick_copy(h, slot, k):
        return remote(
            chosen.at[h, slot, k], picked.at[h, slot, k], pick_sems, (h, slot, k),
            device(z, plane_peers[k], rep),
        )

    for h in range(halves):
        for above in range(2):
            @pl.when(passes_on(above))
            def _():
                line_copy(h, above, 0).start()
    for h in range(halves):
        choose(h, home, z, [x[b, :, half(h)] for b in range(own)])

    group_first = dom * group
    own_first = (dom * reps + rep) * own

    def each(count, body):
        if plan.ahead:
            for i in range(count):
                body(i)
        else:
            lax.fori_loop(0, count, lambda i, c: (body(i), c)[1], 0)

    def span(i):
        return pl.ds(pl.multiple_of(i * TILE, TILE), TILE)

    def build_wide(source, slot):
        def tile(other):
            s = source * plane + lax.rem(p + 2 * plane - 1 - other, plane)
            row, column = tile_row[dom, rep, s], tile_col[dom, rep, s]
            present = row >= 0
            limit = jnp.where(present, tile_count[dom, rep, s], 0)
            row_block = jnp.where(present, row, 0)
            left = across(left_ids[pl.ds(row_block, 1), :])
            right = right_ids[pl.ds(jnp.where(present, column, 0), 1), :]
            bits = bucket(left * (right + 1.0) + 3.0 * right)

            def place(b):
                here = jnp.where(row_block - group_first == b, limit, 0).astype(F32)
                wide[slot, span(b), span(other)] = jnp.where(bits < here, 1.0, 0.0).astype(BF16)

            each(group, place)

        each(plane, tile)

    def build_tall(target):
        s = target * plane + p
        first_own = (s * reps + rep) * own

        def tile(other):
            d = z * plane + lax.rem(p + 2 * plane - 1 - other, plane)
            row, column = tile_row[d, rep, s], tile_col[d, rep, s]
            present = row >= 0
            limit = jnp.where(present, tile_count[d, rep, s], 0)
            left = left_ids[pl.ds(jnp.where(present, row, 0), 1), :]
            right = across(right_ids[pl.ds(jnp.where(present, column, 0), 1), :])
            bits = bucket(left * (right + 1.0) + 3.0 * right)
            for b in range(own):
                here = jnp.where(column - first_own == b, limit, 0).astype(F32)
                tall[target, span(b), span(other)] = jnp.where(bits < here, 1.0, 0.0).astype(BF16)

        each(plane, tile)

    if plan.ahead:
        lax.fori_loop(0, line, lambda i, c: (build_wide(i, i), c)[1], 0)
    lax.fori_loop(0, line, lambda i, c: (build_tall(i), c)[1], 0)

    def count_degrees(s, carry):
        for other in range(reps):
            row, limit = tile_row[dom, other, s], tile_count[dom, other, s]
            carry = tuple(
                value + jnp.where(row == own_first + b, limit, 0) for b, value in enumerate(carry)
            )
        return carry

    degrees = lax.fori_loop(0, plan.doms, count_degrees, (jnp.int32(0),) * own)
    inverse = [
        1.0 / jnp.maximum(jnp.full((8, LANES), degree, jnp.int32).astype(F32), 1.0)[:1]
        for degree in degrees
    ]

    for i in (5, 6, 7):
        loads[i].wait()
    flat_x = x[...].reshape(own * TILE, plan.width_in)
    preact[...] = jnp.dot(flat_x, w_self[...], preferred_element_type=F32)

    def consume(h, slot, source, start):
        for k in range(plane - 1):
            pick_copy(h, slot, k).wait_recv()
        features = picked[h, slot].reshape(plane * TILE, LANES)
        if plan.ahead:
            value = jnp.dot(wide[source], features, preferred_element_type=F32)
            total[h] = value if start else total[h] + value
            return
        build_wide(source, 0)

        def rows(b):
            value = jnp.dot(wide[0, span(b)], features, preferred_element_type=F32)
            total[h, span(b)] = value if start else total[h, span(b)] + value

        each(group, rows)

    def arrive(h, above, k):
        line_copy(h, above, k - 1).wait_recv()

        if k < line - 1:
            @pl.when(passes_on(above))
            def _():
                line_copy(h, above, k).start()

        slot = slot_of(above, k)
        choose(h, slot, spot(above, k), [held[h, slot, b] for b in range(own)])

    def rep_copy(h, peer, slot):
        return remote(
            partial.at[h, peer], landed.at[h, slot], rep_sems, (h, slot), device(z, p, peer)
        )

    def send_partials(h):
        partial[h] = total[h].astype(BF16).reshape(reps, own, TILE, LANES)
        for k, peer in enumerate(rep_peers):
            rep_copy(h, peer, k).start()

    def consume_level(h, k):
        if k == 0:
            consume(h, home, z, True)
            return
        for above, k in levels[k - 1]:
            @pl.when(exists(above, k))
            def _():
                consume(h, slot_of(above, k), spot(above, k), False)

    for k in range(1, line):
        for h in range(halves):
            for above in range(2):
                @pl.when(exists(above, k))
                def _():
                    arrive(h, above, k)
        for h in range(halves):
            consume_level(h, k - 1)
    for h in range(halves):
        consume_level(h, line - 1)
        send_partials(h)

    for h in range(halves):
        for k, peer in enumerate(rep_peers):
            rep_copy(h, peer, k).wait_recv()
        for b in range(own):
            summed = partial[h, rep, b].astype(F32)
            for k in range(reps - 1):
                summed = summed + landed[h, k, b].astype(F32)
            mean[b * TILE : (b + 1) * TILE, half(h)] = (summed * inverse[b]).astype(BF16)
        preact[...] += jnp.dot(
            mean[:, half(h)], w_neigh[half(h), :], preferred_element_type=F32
        )
    value = preact[...]
    logistic = jax.nn.sigmoid(value)
    grad = (cot[...].astype(F32) * logistic * (1.0 + value * (1.0 - logistic))).astype(BF16)

    def spread_copy(h, peer, slot):
        return remote(
            spread[h].at[rep], spread[h].at[rep], spread_sems, (h, slot), device(z, p, peer)
        )

    def spread_arrived(h, k):
        source = lax.rem(rep + reps - k - 1, reps)
        return remote(
            spread[h].at[source], spread[h].at[source], spread_sems, (h, k), device(z, p, source)
        )

    for h in range(halves):
        product = lax.dot_general(grad, w_neigh[half(h), :], OVER_COLS, preferred_element_type=F32)
        for b in range(own):
            spread[h][rep, b] = (product[b * TILE : (b + 1) * TILE] * inverse[b]).astype(BF16)
        for k, peer in enumerate(rep_peers):
            spread_copy(h, peer, k).start()

    both = (x[...].reshape(own * TILE, plan.width_in), mean[...])
    ring_at = col * reps + rep
    ring_peers = []
    for k in range(1, plan.ring):
        other = lax.rem(ring_at + k, plan.ring)
        ring_peers.append(
            (other, device(z, (other // reps) * plan.cores + core, lax.rem(other, reps)))
        )
    core_peers = []
    for k in range(1, plan.cores):
        other = lax.rem(core + k, plan.cores)
        core_peers.append((other, device(z, col * plan.cores + other, rep)))
    far_peers = [(other, device(other, p, rep)) for other in line_peers]

    stages = []
    if plan.split:
        for i, rows in enumerate(both):
            product = lax.dot_general(rows, grad, OVER_ROWS, preferred_element_type=F32)
            terms[i] = product.astype(BF16).reshape(line, plan.ring, plan.strip, plan.width_out)

        def core_copies():
            return [
                remote(terms.at[other], first_in.at[k], core_sems, (k,), to)
                for k, (other, to) in enumerate(core_peers)
            ]

        def far_copies():
            return [
                remote(first.at[other], second_in.at[k], far_sems, (k,), to)
                for k, (other, to) in enumerate(far_peers)
            ]

        def ring_copies():
            return [
                remote(second.at[other], third_in.at[k], ring_sems, (k,), to)
                for k, (other, to) in enumerate(ring_peers)
            ]

        def far_back_copies():
            return [
                remote(final, grads.at[core, z, ring_at], far_back_sems, (k,), to)
                for k, (_, to) in enumerate(far_peers)
            ]

        def ring_back_copies():
            block = grads.at[core, :, ring_at]
            return [
                remote(block, block, ring_back_sems, (k,), to)
                for k, (_, to) in enumerate(ring_peers)
            ]

        def core_back_copies():
            block = grads.at[core]
            return [
                remote(block, block, core_back_sems, (k,), to)
                for k, (_, to) in enumerate(core_peers)
            ]

        def start(copies):
            for copy in copies:
                copy.start()

        def arrived(copies):
            for copy in copies:
                copy.wait_recv()

        def stage_core():
            arrived(core_copies())
            value = terms[core].astype(F32)
            for k in range(len(core_peers)):
                value = value + first_in[k].astype(F32)
            first[...] = value.astype(BF16)
            start(far_copies())

        def stage_far():
            arrived(far_copies())
            value = first[z].astype(F32)
            for k in range(len(far_peers)):
                value = value + second_in[k].astype(F32)
            second[...] = value.astype(BF16)
            start(ring_copies())

        def stage_ring():
            arrived(ring_copies())
            value = second[ring_at].astype(F32)
            for k in range(len(ring_peers)):
                value = value + third_in[k].astype(F32)
            value = (value * scale).astype(BF16)
            final[...] = value
            grads[core, z, ring_at] = value
            start(far_back_copies())

        def stage_ring_back():
            arrived(far_back_copies())
            start(ring_back_copies())

        def stage_core_back():
            arrived(ring_back_copies())
            start(core_back_copies())

        start(core_copies())
        stages = [stage_core, stage_far, stage_ring, stage_ring_back, stage_core_back]
    else:
        for i, rows in enumerate(both):
            grads[i] = lax.dot_general(rows, grad, OVER_ROWS, preferred_element_type=F32)

    def next_stage():
        if stages:
            stages.pop(0)()

    hidden[...] = (value * logistic).astype(BF16)
    back[...] = lax.dot_general(grad, w_self[...], OVER_COLS, preferred_element_type=F32)
    next_stage()

    def pick_back_copy(h, slot, k):
        return remote(
            chosen_back.at[h, slot, k], picked_back.at[h, slot, k], pick_back_sems, (h, slot, k),
            device(z, plane_peers[k], rep),
        )

    def choose_back(h, slot, target):
        def block_for(peer):
            row = tile_row[dom, rep, target * plane + peer]
            offset = jnp.minimum(jnp.maximum(row - group_first, 0), group - 1)
            return spread[h][offset // own, lax.rem(offset, own)]

        for k, peer in enumerate(plane_peers):
            chosen_back[h, slot, k] = block_for(peer)
            pick_back_copy(h, slot, k).start()
        picked_back[h, slot, plane - 1] = block_for(p)

    order = [place for level in reversed(levels) for place in level] + [None]
    for i, place_at in enumerate(order):
        for h in range(halves):
            if i == 0:
                for k in range(reps - 1):
                    spread_arrived(h, k).wait_recv()
            if place_at is None:
                choose_back(h, home, z)
            else:
                @pl.when(exists(*place_at))
                def _():
                    choose_back(h, slot_of(*place_at), spot(*place_at))
        if i + 1 == len(order) - 1 - 2 * (line > 1):
            next_stage()

    def sum_copy(h, above, k):
        slot = slot_of(above, k)
        nearer = slot_of(above, k - 1) if k > 1 else home
        return remote(
            sums_out.at[h, slot], sums_in.at[above, h, nearer], sum_sems, (above, h, k - 1),
            device(z + 2 * above - 1, p, rep),
        )

    def contribution(h, slot, target):
        for k in range(plane - 1):
            pick_back_copy(h, slot, k).wait_recv()
        return jnp.dot(
            tall[target],
            picked_back[h, slot].reshape(plane * TILE, LANES),
            preferred_element_type=F32,
        )

    def pass_sums(h, above, k):
        slot = slot_of(above, k)
        value = contribution(h, slot, spot(above, k))
        sums_out[h, slot] = value.astype(BF16)
        if k < line - 1:
            @pl.when(passes_on(above))
            def _():
                sum_copy(h, above, k + 1).wait_recv()
                sums_out[h, slot] = (
                    sums_out[h, slot].astype(F32) + sums_in[above, h, slot].astype(F32)
                ).astype(BF16)

        sum_copy(h, above, k).start()

    for level in reversed(levels):
        for above, k in level:
            @pl.when(exists(above, k))
            def _():
                for h in range(halves):
                    pass_sums(h, above, k)
        if level is levels[min(1, line - 2)]:
            next_stage()
    next_stage()
    for h in range(halves):
        if h == 1:
            next_stage()
        back[:, half(h)] += contribution(h, home, z)
        for above in range(2 if line > 1 else 0):
            @pl.when(passes_on(above))
            def _():
                sum_copy(h, above, 1).wait_recv()
                back[:, half(h)] += sums_in[above, h, home].astype(F32)
        feat_grad[:, half(h)] = back[:, half(h)].astype(BF16)
    while stages:
        next_stage()
    if plan.split:
        arrived(core_back_copies())

    for h in range(halves):
        for above in range(2):
            @pl.when(passes_on(above))
            def _():
                line_copy(h, above, 0).wait_send()
            for k in range(1, line):
                if k < line - 1:
                    @pl.when(jnp.logical_and(exists(above, k), passes_on(above)))
                    def _():
                        line_copy(h, above, k).wait_send()

                @pl.when(exists(above, k))
                def _():
                    sum_copy(h, above, k).wait_send()
        for slot in range(line):
            for k in range(plane - 1):
                pick_copy(h, slot, k).wait_send()
                pick_back_copy(h, slot, k).wait_send()
        for k, peer in enumerate(rep_peers):
            rep_copy(h, peer, k).wait_send()
            spread_copy(h, peer, k).wait_send()
    if plan.split:
        for copies in (
            core_copies(), ring_copies(), far_copies(),
            far_back_copies(), ring_back_copies(), core_back_copies(),
        ):
            for copy in copies:
                copy.wait_send()


def write_out(hidden, feat_grad, grads, *refs):
    outs, (wide_grads, sems) = refs[:4], refs[4:]
    copies = [
        pltpu.make_async_copy(src, dst, sems.at[i])
        for i, (src, dst) in enumerate(
            zip((hidden, feat_grad, wide_grads.at[0], wide_grads.at[1]), outs)
        )
    ]
    copies[0].start()
    copies[1].start()
    for i in range(2):
        wide_grads[i] = grads[i].astype(F32).reshape(wide_grads.shape[1:])
        copies[2 + i].start()
    for copy in copies:
        copy.wait()


def dma(*shape):
    return pltpu.SemaphoreType.DMA(tuple(max(size, 1) for size in (2,) + shape))


def shards(
    node_feats, node_ids, tile_row, tile_col, tile_count, self_weight, neigh_weight, out_grad
):
    rows, width_in = node_feats.shape
    width_out = self_weight.shape[1]
    plan = Plan(lax.axis_size("dom"), lax.axis_size("rep"), rows, width_in, width_out)
    line, plane, reps, own, halves = plan.line, plan.plane, plan.reps, plan.own, plan.halves
    scale = 1.0 / math.sqrt(rows * plan.doms * reps)
    id_rows = node_ids.shape[0] // TILE

    def buffer(*shape, dtype=BF16):
        return pltpu.VMEM(tuple(max(size, 1) for size in shape), dtype)

    tile = (TILE, LANES)
    tables = pltpu.SMEM(tile_row.shape, jnp.int32)
    scratch = [
        tables,
        tables,
        tables,
        buffer(id_rows, TILE, dtype=jnp.int32),
        buffer(own, TILE, width_in),
        buffer(rows, width_out),
        buffer(width_in, width_out),
        buffer(width_in, width_out),
        buffer(id_rows, TILE, dtype=F32),
        buffer(id_rows, TILE, dtype=F32),
        buffer(line if plan.ahead else 1, plan.group * TILE, plane * TILE),
        buffer(line, own * TILE, plane * TILE),
        buffer(halves, line, own, *tile),
        buffer(halves, line, plane, *tile),
        buffer(halves, line, plane, *tile),
        buffer(halves, plan.group * TILE, LANES, dtype=F32),
        buffer(halves, reps, own, *tile),
        buffer(halves, reps - 1, own, *tile),
        buffer(rows, width_in),
        buffer(rows, width_out, dtype=F32),
        buffer(rows, width_in, dtype=F32),
        *[buffer(reps, own, *tile) for _ in range(halves)],
        buffer(halves, line, plane, *tile),
        buffer(halves, line, plane, *tile),
        buffer(halves, line, own * TILE, LANES),
        buffer(2, halves, line, own * TILE, LANES),
    ]
    strip = (plan.strip, width_out)
    if plan.split:
        scratch += [
            buffer(plan.cores, line, plan.ring, *strip),
            buffer(plan.cores - 1, line, plan.ring, *strip),
            buffer(line, plan.ring, *strip),
            buffer(line - 1, plan.ring, *strip),
            buffer(plan.ring, *strip),
            buffer(plan.ring - 1, *strip),
            buffer(*strip),
        ]
    scratch += [
        pltpu.SemaphoreType.DMA((8,)),
        dma(2, halves, line),
        dma(halves, line, plane),
        dma(halves, reps - 1),
        dma(halves, reps - 1),
        dma(halves, line, plane),
        dma(2, halves, line),
    ]
    if plan.split:
        scratch += [
            dma(plan.cores - 1), dma(line - 1), dma(plan.ring - 1),
            dma(line - 1), dma(plan.ring - 1), dma(plan.cores - 1),
        ]
        grads_shape = jax.ShapeDtypeStruct((plan.cores, line, plan.ring, *strip), BF16)
    else:
        grads_shape = jax.ShapeDtypeStruct((2, width_in, width_out), F32)
    vmem, anywhere = pl.BlockSpec(memory_space=pltpu.VMEM), pl.BlockSpec(memory_space=pl.ANY)
    hidden_out, feat_grad, grads = pl.pallas_call(
        functools.partial(fused, plan, scale),
        out_shape=(
            pltpu.VMEM((rows, width_out), BF16),
            pltpu.VMEM((rows, width_in), BF16),
            pltpu.VMEM(grads_shape.shape, grads_shape.dtype),
        ),
        in_specs=[anywhere] * 8,
        out_specs=(vmem,) * 3,
        scratch_shapes=scratch,
        compiler_params=pltpu.CompilerParams(collective_id=1, has_side_effects=True),
    )(
        tile_row,
        tile_col,
        tile_count,
        node_ids.reshape(id_rows, TILE),
        node_feats.reshape(own, TILE, width_in),
        out_grad,
        self_weight,
        neigh_weight,
    )
    if not plan.split:
        grads = lax.psum(grads, ("dom", "rep")) * scale
        return hidden_out, feat_grad, grads[0], grads[1]
    grad_shape = jax.ShapeDtypeStruct((width_in, width_out), F32)
    return pl.pallas_call(
        write_out,
        out_shape=(
            jax.ShapeDtypeStruct((rows, width_out), BF16),
            jax.ShapeDtypeStruct((rows, width_in), BF16),
            grad_shape,
            grad_shape,
        ),
        in_specs=[vmem] * 3,
        out_specs=(anywhere,) * 4,
        scratch_shapes=[
            buffer(2, width_in, width_out, dtype=F32),
            pltpu.SemaphoreType.DMA((4,)),
        ],
        compiler_params=pltpu.CompilerParams(vmem_limit_bytes=2**23),
    )(hidden_out, feat_grad, grads)


def solution(mesh):
    placed = (P(("dom", "rep"), None), P(), P(), P(), P(), P(), P(), P(("dom", "rep"), None))
    return jax.shard_map(
        shards,
        mesh=mesh,
        in_specs=placed,
        out_specs=(P(("dom", "rep"), None), P(("dom", "rep"), None), P(), P()),
        check_vma=False,
    )
```

```python
import functools
import math

import jax
import jax.numpy as jnp
from jax import lax
from jax.experimental import pallas as pl
from jax.experimental.pallas import tpu as pltpu
from jax.sharding import PartitionSpec as P

TILE = 128
LANES = 128
HASH = 4099.0

MESH = pl.DeviceIdType.MESH
OVER_ROWS = (((0,), (0,)), ((), ()))
OVER_COLS = (((1,), (1,)), ((), ()))
BF16 = jnp.bfloat16
F32 = jnp.float32


def modulo(value, base):
    quotient = jnp.floor(value * ((1.0 - 2.0**-20) / base))
    left = value - quotient * base
    return jnp.where(left >= base, left - base, left)


def across(row):
    return jnp.broadcast_to(row, (TILE, TILE)).T


def bucket(hashed):
    left = modulo(hashed, HASH)
    return left - jnp.floor(left * (1.0 / TILE)) * TILE


class Plan:
    def __init__(self, dom_total, rep_total, rows, width_in, width_out):
        self.line = math.gcd(dom_total, 4)
        self.plane = dom_total // self.line
        self.cores = math.gcd(self.plane, 2)
        self.cols = self.plane // self.cores
        self.reps = rep_total
        self.doms = dom_total
        self.own = rows // TILE
        self.group = self.own * rep_total
        self.halves = width_in // LANES
        self.width_in, self.width_out = width_in, width_out
        self.ring = self.cols * rep_total
        self.strip = 2 * width_in // (self.cores * self.ring * self.line)
        self.split = self.strip % 16 == 0 and self.cores == 2
        self.ahead = self.line * self.group * self.plane * TILE * TILE * 2 <= 2**23


def fused(plan, scale, *refs):
    refs = list(refs)

    def take(count):
        out, refs[:count] = refs[:count], []
        return out

    line, plane, reps, own, group, halves = (
        plan.line, plan.plane, plan.reps, plan.own, plan.group, plan.halves,
    )
    given = take(8)
    hidden, feat_grad, grads = take(3)
    inputs = take(8)
    tile_row, tile_col, tile_count, ids, x, cot, w_self, w_neigh = inputs
    left_ids, right_ids, wide, tall = take(4)
    held, chosen, picked, total, partial, landed, mean, preact, back = take(9)
    spread = take(halves)
    picked_back, chosen_back, sums_out, sums_in = take(4)
    if plan.split:
        terms, first_in, first, second_in, second, third_in, final = take(7)
    (load_sems,) = take(1)
    line_sems, pick_sems, rep_sems, spread_sems, pick_back_sems, sum_sems = take(6)
    if plan.split:
        core_sems, far_sems, ring_sems, far_back_sems, ring_back_sems, core_back_sems = take(6)

    dom, rep = lax.axis_index("dom"), lax.axis_index("rep")
    z, p = dom // plane, lax.rem(dom, plane)

    def device(zz, pp, rr):
        return (zz * plane + pp, rr)

    def remote(src, dst, sems, index, target):
        return pltpu.make_async_remote_copy(
            src_ref=src,
            dst_ref=dst,
            send_sem=sems.at[(0,) + index],
            recv_sem=sems.at[(1,) + index],
            device_id=target,
            device_id_type=MESH,
        )

    line_peers = [lax.rem(z + k, line) for k in range(1, line)]
    plane_peers = [lax.rem(p + k, plane) for k in range(1, plane)]
    rep_peers = [lax.rem(rep + k, reps) for k in range(1, reps)]
    col, core = p // plan.cores, lax.rem(p, plan.cores)

    everyone = [device(other, p, rep) for other in line_peers]
    everyone += [device(z, other, rep) for other in plane_peers]
    for k in range(plan.cols):
        other = lax.rem(col + k, plan.cols) * plan.cores + core
        everyone += [device(z, other, peer) for peer in rep_peers]
    loads = [
        pltpu.make_async_copy(src, dst, load_sems.at[i])
        for i, (src, dst) in enumerate(zip(given, inputs))
    ]
    for i in (4, 1, 3, 0, 2, 6, 7, 5):
        loads[i].start()
    barrier = pltpu.get_barrier_semaphore()
    for peer in everyone:
        pl.semaphore_signal(barrier, inc=1, device_id=peer, device_id_type=MESH)

    for i in (0, 1, 2, 3, 4):
        loads[i].wait()
    node = ids[...].astype(F32)
    left_ids[...] = modulo(node, 4093.0)
    right_ids[...] = modulo(node, 4091.0)

    home = line - 1
    levels = [[(above, k) for above in range(2)] for k in range(1, line)]

    def slot_of(above, k):
        return line - 1 - k if above else k - 1

    def spot(above, k):
        return z + k if above else z - k

    def exists(above, k):
        return z < line - k if above else z >= k

    def half(h):
        return slice(h * LANES, (h + 1) * LANES)

    def passes_on(above):
        return z >= 1 if above else z < line - 1

    def line_copy(h, above, k):
        slot = slot_of(above, k + 1)
        src = held.at[h, slot_of(above, k)] if k else x.at[:, :, half(h)]
        return remote(
            src, held.at[h, slot], line_sems, (above, h, k), device(z + 1 - 2 * above, p, rep)
        )

    pl.semaphore_wait(barrier, len(everyone))

    def choose(h, slot, source, blocks):
        first_own = ((source * plane + p) * reps + rep) * own

        def block_for(d):
            offset = tile_col[d, rep, source * plane + p] - first_own
            value = blocks[0]
            for b in range(1, own):
                value = lax.select(offset == b, blocks[b], value)
            return value

        for k, peer in enumerate(plane_peers):
            chosen[h, slot, k] = block_for(z * plane + peer)
            pick_copy(h, slot, k).start()
        picked[h, slot, plane - 1] = block_for(dom)

    def pick_copy(h, slot, k):
        return remote(
            chosen.at[h, slot, k], picked.at[h, slot, k], pick_sems, (h, slot, k),
            device(z, plane_peers[k], rep),
        )

    for h in range(halves):
        for above in range(2):
            @pl.when(passes_on(above))
            def _():
                line_copy(h, above, 0).start()
    for h in range(halves):
        choose(h, home, z, [x[b, :, half(h)] for b in range(own)])

    group_first = dom * group
    own_first = (dom * reps + rep) * own

    def each(count, body):
        if plan.ahead:
            for i in range(count):
                body(i)
        else:
            lax.fori_loop(0, count, lambda i, c: (body(i), c)[1], 0)

    def span(i):
        return pl.ds(pl.multiple_of(i * TILE, TILE), TILE)

    def build_wide(source, slot):
        def tile(other):
            s = source * plane + lax.rem(p + 2 * plane - 1 - other, plane)
            row, column = tile_row[dom, rep, s], tile_col[dom, rep, s]
            present = row >= 0
            limit = jnp.where(present, tile_count[dom, rep, s], 0)
            row_block = jnp.where(present, row, 0)
            left = across(left_ids[pl.ds(row_block, 1), :])
            right = right_ids[pl.ds(jnp.where(present, column, 0), 1), :]
            bits = bucket(left * (right + 1.0) + 3.0 * right)

            def place(b):
                here = jnp.where(row_block - group_first == b, limit, 0).astype(F32)
                wide[slot, span(b), span(other)] = jnp.where(bits < here, 1.0, 0.0).astype(BF16)

            each(group, place)

        each(plane, tile)

    def build_tall(target):
        s = target * plane + p
        first_own = (s * reps + rep) * own

        def tile(other):
            d = z * plane + lax.rem(p + 2 * plane - 1 - other, plane)
            row, column = tile_row[d, rep, s], tile_col[d, rep, s]
            present = row >= 0
            limit = jnp.where(present, tile_count[d, rep, s], 0)
            left = left_ids[pl.ds(jnp.where(present, row, 0), 1), :]
            right = across(right_ids[pl.ds(jnp.where(present, column, 0), 1), :])
            bits = bucket(left * (right + 1.0) + 3.0 * right)
            for b in range(own):
                here = jnp.where(column - first_own == b, limit, 0).astype(F32)
                tall[target, span(b), span(other)] = jnp.where(bits < here, 1.0, 0.0).astype(BF16)

        each(plane, tile)

    if plan.ahead:
        lax.fori_loop(0, line, lambda i, c: (build_wide(i, i), c)[1], 0)
    lax.fori_loop(0, line, lambda i, c: (build_tall(i), c)[1], 0)

    def count_degrees(s, carry):
        for other in range(reps):
            row, limit = tile_row[dom, other, s], tile_count[dom, other, s]
            carry = tuple(
                value + jnp.where(row == own_first + b, limit, 0) for b, value in enumerate(carry)
            )
        return carry

    degrees = lax.fori_loop(0, plan.doms, count_degrees, (jnp.int32(0),) * own)
    inverse = [
        1.0 / jnp.maximum(jnp.full((8, LANES), degree, jnp.int32).astype(F32), 1.0)[:1]
        for degree in degrees
    ]

    for i in (5, 6, 7):
        loads[i].wait()
    flat_x = x[...].reshape(own * TILE, plan.width_in)
    preact[...] = jnp.dot(flat_x, w_self[...], preferred_element_type=F32)

    def consume(h, slot, source, start):
        for k in range(plane - 1):
            pick_copy(h, slot, k).wait_recv()
        features = picked[h, slot].reshape(plane * TILE, LANES)
        if plan.ahead:
            value = jnp.dot(wide[source], features, preferred_element_type=F32)
            total[h] = value if start else total[h] + value
            return
        build_wide(source, 0)

        def rows(b):
            value = jnp.dot(wide[0, span(b)], features, preferred_element_type=F32)
            total[h, span(b)] = value if start else total[h, span(b)] + value

        each(group, rows)

    def arrive(h, above, k):
        line_copy(h, above, k - 1).wait_recv()

        if k < line - 1:
            @pl.when(passes_on(above))
            def _():
                line_copy(h, above, k).start()

        slot = slot_of(above, k)
        choose(h, slot, spot(above, k), [held[h, slot, b] for b in range(own)])

    def rep_copy(h, peer, slot):
        return remote(
            partial.at[h, peer], landed.at[h, slot], rep_sems, (h, slot), device(z, p, peer)
        )

    def send_partials(h):
        partial[h] = total[h].astype(BF16).reshape(reps, own, TILE, LANES)
        for k, peer in enumerate(rep_peers):
            rep_copy(h, peer, k).start()

    def consume_level(h, k):
        if k == 0:
            consume(h, home, z, True)
            return
        for above, k in levels[k - 1]:
            @pl.when(exists(above, k))
            def _():
                consume(h, slot_of(above, k), spot(above, k), False)

    for k in range(1, line):
        for h in range(halves):
            for above in range(2):
                @pl.when(exists(above, k))
                def _():
                    arrive(h, above, k)
        for h in range(halves):
            consume_level(h, k - 1)
    for h in range(halves):
        consume_level(h, line - 1)
        send_partials(h)

    for h in range(halves):
        for k, peer in enumerate(rep_peers):
            rep_copy(h, peer, k).wait_recv()
        for b in range(own):
            summed = partial[h, rep, b].astype(F32)
            for k in range(reps - 1):
                summed = summed + landed[h, k, b].astype(F32)
            mean[b * TILE : (b + 1) * TILE, half(h)] = (summed * inverse[b]).astype(BF16)
        preact[...] += jnp.dot(
            mean[:, half(h)], w_neigh[half(h), :], preferred_element_type=F32
        )
    value = preact[...]
    logistic = jax.nn.sigmoid(value)
    grad = (cot[...].astype(F32) * logistic * (1.0 + value * (1.0 - logistic))).astype(BF16)

    def spread_copy(h, peer, slot):
        return remote(
            spread[h].at[rep], spread[h].at[rep], spread_sems, (h, slot), device(z, p, peer)
        )

    def spread_arrived(h, k):
        source = lax.rem(rep + reps - k - 1, reps)
        return remote(
            spread[h].at[source], spread[h].at[source], spread_sems, (h, k), device(z, p, source)
        )

    for h in range(halves):
        product = lax.dot_general(grad, w_neigh[half(h), :], OVER_COLS, preferred_element_type=F32)
        for b in range(own):
            spread[h][rep, b] = (product[b * TILE : (b + 1) * TILE] * inverse[b]).astype(BF16)
        for k, peer in enumerate(rep_peers):
            spread_copy(h, peer, k).start()

    both = (x[...].reshape(own * TILE, plan.width_in), mean[...])
    ring_at = col * reps + rep
    ring_peers = []
    for k in range(1, plan.ring):
        other = lax.rem(ring_at + k, plan.ring)
        ring_peers.append(
            (other, device(z, (other // reps) * plan.cores + core, lax.rem(other, reps)))
        )
    core_peers = []
    for k in range(1, plan.cores):
        other = lax.rem(core + k, plan.cores)
        core_peers.append((other, device(z, col * plan.cores + other, rep)))
    far_peers = [(other, device(other, p, rep)) for other in line_peers]

    stages = []
    if plan.split:
        for i, rows in enumerate(both):
            product = lax.dot_general(rows, grad, OVER_ROWS, preferred_element_type=F32)
            terms[i] = product.astype(BF16).reshape(line, plan.ring, plan.strip, plan.width_out)

        def core_copies():
            return [
                remote(terms.at[other], first_in.at[k], core_sems, (k,), to)
                for k, (other, to) in enumerate(core_peers)
            ]

        def far_copies():
            return [
                remote(first.at[other], second_in.at[k], far_sems, (k,), to)
                for k, (other, to) in enumerate(far_peers)
            ]

        def ring_copies():
            return [
                remote(second.at[other], third_in.at[k], ring_sems, (k,), to)
                for k, (other, to) in enumerate(ring_peers)
            ]

        def far_back_copies():
            return [
                remote(final, grads.at[core, z, ring_at], far_back_sems, (k,), to)
                for k, (_, to) in enumerate(far_peers)
            ]

        def ring_back_copies():
            block = grads.at[core, :, ring_at]
            return [
                remote(block, block, ring_back_sems, (k,), to)
                for k, (_, to) in enumerate(ring_peers)
            ]

        def core_back_copies():
            block = grads.at[core]
            return [
                remote(block, block, core_back_sems, (k,), to)
                for k, (_, to) in enumerate(core_peers)
            ]

        def start(copies):
            for copy in copies:
                copy.start()

        def arrived(copies):
            for copy in copies:
                copy.wait_recv()

        def stage_core():
            arrived(core_copies())
            value = terms[core].astype(F32)
            for k in range(len(core_peers)):
                value = value + first_in[k].astype(F32)
            first[...] = value.astype(BF16)
            start(far_copies())

        def stage_far():
            arrived(far_copies())
            value = first[z].astype(F32)
            for k in range(len(far_peers)):
                value = value + second_in[k].astype(F32)
            second[...] = value.astype(BF16)
            start(ring_copies())

        def stage_ring():
            arrived(ring_copies())
            value = second[ring_at].astype(F32)
            for k in range(len(ring_peers)):
                value = value + third_in[k].astype(F32)
            value = (value * scale).astype(BF16)
            final[...] = value
            grads[core, z, ring_at] = value
            start(far_back_copies())

        def stage_ring_back():
            arrived(far_back_copies())
            start(ring_back_copies())

        def stage_core_back():
            arrived(ring_back_copies())
            start(core_back_copies())

        start(core_copies())
        stages = [stage_core, stage_far, stage_ring, stage_ring_back, stage_core_back]
    else:
        for i, rows in enumerate(both):
            grads[i] = lax.dot_general(rows, grad, OVER_ROWS, preferred_element_type=F32)

    def next_stage():
        if stages:
            stages.pop(0)()

    hidden[...] = (value * logistic).astype(BF16)
    back[...] = lax.dot_general(grad, w_self[...], OVER_COLS, preferred_element_type=F32)
    next_stage()

    def pick_back_copy(h, slot, k):
        return remote(
            chosen_back.at[h, slot, k], picked_back.at[h, slot, k], pick_back_sems, (h, slot, k),
            device(z, plane_peers[k], rep),
        )

    def choose_back(h, slot, target):
        def block_for(peer):
            row = tile_row[dom, rep, target * plane + peer]
            offset = jnp.minimum(jnp.maximum(row - group_first, 0), group - 1)
            return spread[h][offset // own, lax.rem(offset, own)]

        for k, peer in enumerate(plane_peers):
            chosen_back[h, slot, k] = block_for(peer)
            pick_back_copy(h, slot, k).start()
        picked_back[h, slot, plane - 1] = block_for(p)

    for h in range(halves):
        for k in range(reps - 1):
            spread_arrived(h, k).wait_recv()
        for above, k in (levels[-1] if levels else []):
            @pl.when(exists(above, k))
            def _():
                choose_back(h, slot_of(above, k), spot(above, k))

    def choose_level(level):
        for above, k in level:
            @pl.when(exists(above, k))
            def _():
                for h in range(halves):
                    choose_back(h, slot_of(above, k), spot(above, k))

    def sum_copy(h, above, k):
        slot = slot_of(above, k)
        nearer = slot_of(above, k - 1) if k > 1 else home
        return remote(
            sums_out.at[h, slot], sums_in.at[above, h, nearer], sum_sems, (above, h, k - 1),
            device(z + 2 * above - 1, p, rep),
        )

    def contribution(h, slot, target):
        for k in range(plane - 1):
            pick_back_copy(h, slot, k).wait_recv()
        return jnp.dot(
            tall[target],
            picked_back[h, slot].reshape(plane * TILE, LANES),
            preferred_element_type=F32,
        )

    def pass_sums(h, above, k):
        slot = slot_of(above, k)
        value = contribution(h, slot, spot(above, k))
        sums_out[h, slot] = value.astype(BF16)
        if k < line - 1:
            @pl.when(passes_on(above))
            def _():
                sum_copy(h, above, k + 1).wait_recv()
                sums_out[h, slot] = (
                    sums_out[h, slot].astype(F32) + sums_in[above, h, slot].astype(F32)
                ).astype(BF16)

        sum_copy(h, above, k).start()

    upper = 2 * z >= line

    def pass_level(level):
        for above, k, turn in [(1, k, upper) for _, k in level[:1]] + [
            (0, k, None) for _, k in level[:1]
        ] + [(1, k, jnp.logical_not(upper)) for _, k in level[:1]]:
            here = exists(above, k)

            @pl.when(here if turn is None else jnp.logical_and(here, turn))
            def _():
                for h in range(halves):
                    pass_sums(h, above, k)

    turn = stages.pop(1) if len(stages) > 1 else None
    for level in reversed(levels[-2:-1]):
        choose_level(level)
    for level in levels[-1:]:
        pass_level(level)
    next_stage()
    for level in reversed(levels[:-2]):
        choose_level(level)
    for h in range(halves):
        choose_back(h, home, z)
    rest = levels[:-1]
    if turn:
        turn()
    for level in rest[-1:]:
        pass_level(level)
    next_stage()
    for level in reversed(rest[:-1]):
        pass_level(level)
    next_stage()
    for h in range(halves):
        back[:, half(h)] += contribution(h, home, z)
        for above in range(2 if line > 1 else 0):
            @pl.when(passes_on(above))
            def _():
                sum_copy(h, above, 1).wait_recv()
                back[:, half(h)] += sums_in[above, h, home].astype(F32)
        feat_grad[:, half(h)] = back[:, half(h)].astype(BF16)
    while stages:
        next_stage()
    if plan.split:
        arrived(core_back_copies())

    for h in range(halves):
        for above in range(2):
            @pl.when(passes_on(above))
            def _():
                line_copy(h, above, 0).wait_send()
            for k in range(1, line):
                if k < line - 1:
                    @pl.when(jnp.logical_and(exists(above, k), passes_on(above)))
                    def _():
                        line_copy(h, above, k).wait_send()

                @pl.when(exists(above, k))
                def _():
                    sum_copy(h, above, k).wait_send()
        for slot in range(line):
            for k in range(plane - 1):
                pick_copy(h, slot, k).wait_send()
                pick_back_copy(h, slot, k).wait_send()
        for k, peer in enumerate(rep_peers):
            rep_copy(h, peer, k).wait_send()
            spread_copy(h, peer, k).wait_send()
    if plan.split:
        for copies in (
            core_copies(), ring_copies(), far_copies(),
            far_back_copies(), ring_back_copies(), core_back_copies(),
        ):
            for copy in copies:
                copy.wait_send()


def write_out(hidden, feat_grad, grads, *refs):
    outs, (wide_grads, sems) = refs[:4], refs[4:]
    copies = [
        pltpu.make_async_copy(src, dst, sems.at[i])
        for i, (src, dst) in enumerate(
            zip((hidden, feat_grad, wide_grads.at[0], wide_grads.at[1]), outs)
        )
    ]
    copies[0].start()
    copies[1].start()
    for i in range(2):
        wide_grads[i] = grads[i].astype(F32).reshape(wide_grads.shape[1:])
        copies[2 + i].start()
    for copy in copies:
        copy.wait()


def dma(*shape):
    return pltpu.SemaphoreType.DMA(tuple(max(size, 1) for size in (2,) + shape))


def shards(
    node_feats, node_ids, tile_row, tile_col, tile_count, self_weight, neigh_weight, out_grad
):
    rows, width_in = node_feats.shape
    width_out = self_weight.shape[1]
    plan = Plan(lax.axis_size("dom"), lax.axis_size("rep"), rows, width_in, width_out)
    line, plane, reps, own, halves = plan.line, plan.plane, plan.reps, plan.own, plan.halves
    scale = 1.0 / math.sqrt(rows * plan.doms * reps)
    id_rows = node_ids.shape[0] // TILE

    def buffer(*shape, dtype=BF16):
        return pltpu.VMEM(tuple(max(size, 1) for size in shape), dtype)

    tile = (TILE, LANES)
    tables = pltpu.SMEM(tile_row.shape, jnp.int32)
    scratch = [
        tables,
        tables,
        tables,
        buffer(id_rows, TILE, dtype=jnp.int32),
        buffer(own, TILE, width_in),
        buffer(rows, width_out),
        buffer(width_in, width_out),
        buffer(width_in, width_out),
        buffer(id_rows, TILE, dtype=F32),
        buffer(id_rows, TILE, dtype=F32),
        buffer(line if plan.ahead else 1, plan.group * TILE, plane * TILE),
        buffer(line, own * TILE, plane * TILE),
        buffer(halves, line, own, *tile),
        buffer(halves, line, plane, *tile),
        buffer(halves, line, plane, *tile),
        buffer(halves, plan.group * TILE, LANES, dtype=F32),
        buffer(halves, reps, own, *tile),
        buffer(halves, reps - 1, own, *tile),
        buffer(rows, width_in),
        buffer(rows, width_out, dtype=F32),
        buffer(rows, width_in, dtype=F32),
        *[buffer(reps, own, *tile) for _ in range(halves)],
        buffer(halves, line, plane, *tile),
        buffer(halves, line, plane, *tile),
        buffer(halves, line, own * TILE, LANES),
        buffer(2, halves, line, own * TILE, LANES),
    ]
    strip = (plan.strip, width_out)
    if plan.split:
        scratch += [
            buffer(plan.cores, line, plan.ring, *strip),
            buffer(plan.cores - 1, line, plan.ring, *strip),
            buffer(line, plan.ring, *strip),
            buffer(line - 1, plan.ring, *strip),
            buffer(plan.ring, *strip),
            buffer(plan.ring - 1, *strip),
            buffer(*strip),
        ]
    scratch += [
        pltpu.SemaphoreType.DMA((8,)),
        dma(2, halves, line),
        dma(halves, line, plane),
        dma(halves, reps - 1),
        dma(halves, reps - 1),
        dma(halves, line, plane),
        dma(2, halves, line),
    ]
    if plan.split:
        scratch += [
            dma(plan.cores - 1), dma(line - 1), dma(plan.ring - 1),
            dma(line - 1), dma(plan.ring - 1), dma(plan.cores - 1),
        ]
        grads_shape = jax.ShapeDtypeStruct((plan.cores, line, plan.ring, *strip), BF16)
    else:
        grads_shape = jax.ShapeDtypeStruct((2, width_in, width_out), F32)
    vmem, anywhere = pl.BlockSpec(memory_space=pltpu.VMEM), pl.BlockSpec(memory_space=pl.ANY)
    hidden_out, feat_grad, grads = pl.pallas_call(
        functools.partial(fused, plan, scale),
        out_shape=(
            pltpu.VMEM((rows, width_out), BF16),
            pltpu.VMEM((rows, width_in), BF16),
            pltpu.VMEM(grads_shape.shape, grads_shape.dtype),
        ),
        in_specs=[anywhere] * 8,
        out_specs=(vmem,) * 3,
        scratch_shapes=scratch,
        compiler_params=pltpu.CompilerParams(collective_id=1, has_side_effects=True),
    )(
        tile_row,
        tile_col,
        tile_count,
        node_ids.reshape(id_rows, TILE),
        node_feats.reshape(own, TILE, width_in),
        out_grad,
        self_weight,
        neigh_weight,
    )
    if not plan.split:
        grads = lax.psum(grads, ("dom", "rep")) * scale
        return hidden_out, feat_grad, grads[0], grads[1]
    grad_shape = jax.ShapeDtypeStruct((width_in, width_out), F32)
    return pl.pallas_call(
        write_out,
        out_shape=(
            jax.ShapeDtypeStruct((rows, width_out), BF16),
            jax.ShapeDtypeStruct((rows, width_in), BF16),
            grad_shape,
            grad_shape,
        ),
        in_specs=[vmem] * 3,
        out_specs=(anywhere,) * 4,
        scratch_shapes=[
            buffer(2, width_in, width_out, dtype=F32),
            pltpu.SemaphoreType.DMA((4,)),
        ],
        compiler_params=pltpu.CompilerParams(vmem_limit_bytes=2**23),
    )(hidden_out, feat_grad, grads)


def solution(mesh):
    placed = (P(("dom", "rep"), None), P(), P(), P(), P(), P(), P(), P(("dom", "rep"), None))
    return jax.shard_map(
        shards,
        mesh=mesh,
        in_specs=placed,
        out_specs=(P(("dom", "rep"), None), P(("dom", "rep"), None), P(), P()),
        check_vma=False,
    )
```

```python
import functools
import math

import jax
import jax.numpy as jnp
from jax import lax
from jax.experimental import pallas as pl
from jax.experimental.pallas import tpu as pltpu
from jax.sharding import PartitionSpec as P

TILE = 128
LANES = 128
HASH = 4099.0

MESH = pl.DeviceIdType.MESH
OVER_ROWS = (((0,), (0,)), ((), ()))
OVER_COLS = (((1,), (1,)), ((), ()))
BF16 = jnp.bfloat16
F32 = jnp.float32


def modulo(value, base):
    quotient = jnp.floor(value * ((1.0 - 2.0**-20) / base))
    left = value - quotient * base
    return jnp.where(left >= base, left - base, left)


def across(row):
    return jnp.broadcast_to(row, (TILE, TILE)).T


def bucket(hashed):
    left = modulo(hashed, HASH)
    return left - jnp.floor(left * (1.0 / TILE)) * TILE


class Plan:
    def __init__(self, dom_total, rep_total, rows, width_in, width_out):
        self.line = math.gcd(dom_total, 4)
        self.plane = dom_total // self.line
        self.cores = math.gcd(self.plane, 2)
        self.cols = self.plane // self.cores
        self.reps = rep_total
        self.doms = dom_total
        self.own = rows // TILE
        self.group = self.own * rep_total
        self.halves = width_in // LANES
        self.width_in, self.width_out = width_in, width_out
        self.ring = self.cols * rep_total
        self.strip = 2 * width_in // (self.cores * self.ring * self.line)
        self.split = self.strip % 16 == 0 and self.cores == 2
        self.ahead = self.line * self.group * self.plane * TILE * TILE * 2 <= 2**23


def fused(plan, scale, *refs):
    refs = list(refs)

    def take(count):
        out, refs[:count] = refs[:count], []
        return out

    line, plane, reps, own, group, halves = (
        plan.line, plan.plane, plan.reps, plan.own, plan.group, plan.halves,
    )
    given = take(8)
    hidden, feat_grad, grads = take(3)
    inputs = take(8)
    tile_row, tile_col, tile_count, ids, x, cot, w_self, w_neigh = inputs
    left_ids, right_ids, wide, tall = take(4)
    held, chosen, picked, total, partial, landed, mean, preact, back = take(9)
    spread = take(halves)
    picked_back, chosen_back, sums_out, sums_in = take(4)
    if plan.split:
        terms, first_in, first, second_in, second, third_in, final = take(7)
    (load_sems,) = take(1)
    line_sems, pick_sems, rep_sems, spread_sems, pick_back_sems, sum_sems = take(6)
    if plan.split:
        core_sems, far_sems, ring_sems, far_back_sems, ring_back_sems, core_back_sems = take(6)

    dom, rep = lax.axis_index("dom"), lax.axis_index("rep")
    z, p = dom // plane, lax.rem(dom, plane)

    def device(zz, pp, rr):
        return (zz * plane + pp, rr)

    def remote(src, dst, sems, index, target):
        return pltpu.make_async_remote_copy(
            src_ref=src,
            dst_ref=dst,
            send_sem=sems.at[(0,) + index],
            recv_sem=sems.at[(1,) + index],
            device_id=target,
            device_id_type=MESH,
        )

    line_peers = [lax.rem(z + k, line) for k in range(1, line)]
    plane_peers = [lax.rem(p + k, plane) for k in range(1, plane)]
    rep_peers = [lax.rem(rep + k, reps) for k in range(1, reps)]
    col, core = p // plan.cores, lax.rem(p, plan.cores)

    everyone = [device(other, p, rep) for other in line_peers]
    everyone += [device(z, other, rep) for other in plane_peers]
    for k in range(plan.cols):
        other = lax.rem(col + k, plan.cols) * plan.cores + core
        everyone += [device(z, other, peer) for peer in rep_peers]
    loads = [
        pltpu.make_async_copy(src, dst, load_sems.at[i])
        for i, (src, dst) in enumerate(zip(given, inputs))
    ]
    for i in (4, 1, 3, 0, 2, 6, 7, 5):
        loads[i].start()
    barrier = pltpu.get_barrier_semaphore()
    for peer in everyone:
        pl.semaphore_signal(barrier, inc=1, device_id=peer, device_id_type=MESH)


    home = line - 1
    levels = [[(above, k) for above in range(2)] for k in range(1, line)]

    def slot_of(above, k):
        return line - 1 - k if above else k - 1

    def spot(above, k):
        return z + k if above else z - k

    def exists(above, k):
        return z < line - k if above else z >= k

    def half(h):
        return slice(h * LANES, (h + 1) * LANES)

    def passes_on(above):
        return z >= 1 if above else z < line - 1

    def line_copy(h, above, k):
        slot = slot_of(above, k + 1)
        src = held.at[h, slot_of(above, k)] if k else x.at[:, :, half(h)]
        return remote(
            src, held.at[h, slot], line_sems, (above, h, k), device(z + 1 - 2 * above, p, rep)
        )

    loads[4].wait()
    pl.semaphore_wait(barrier, len(everyone))

    def choose(h, slot, source, blocks):
        first_own = ((source * plane + p) * reps + rep) * own

        def block_for(d):
            offset = tile_col[d, rep, source * plane + p] - first_own
            value = blocks[0]
            for b in range(1, own):
                value = lax.select(offset == b, blocks[b], value)
            return value

        for k, peer in enumerate(plane_peers):
            chosen[h, slot, k] = block_for(z * plane + peer)
            pick_copy(h, slot, k).start()
        picked[h, slot, plane - 1] = block_for(dom)

    def pick_copy(h, slot, k):
        return remote(
            chosen.at[h, slot, k], picked.at[h, slot, k], pick_sems, (h, slot, k),
            device(z, plane_peers[k], rep),
        )

    for h in range(halves):
        for above in range(2):
            @pl.when(passes_on(above))
            def _():
                line_copy(h, above, 0).start()
    for i in range(4):
        loads[i].wait()
    node = ids[...].astype(F32)
    left_ids[...] = modulo(node, 4093.0)
    right_ids[...] = modulo(node, 4091.0)
    for h in range(halves):
        choose(h, home, z, [x[b, :, half(h)] for b in range(own)])

    group_first = dom * group
    own_first = (dom * reps + rep) * own

    def each(count, body):
        if plan.ahead:
            for i in range(count):
                body(i)
        else:
            lax.fori_loop(0, count, lambda i, c: (body(i), c)[1], 0)

    def span(i):
        return pl.ds(pl.multiple_of(i * TILE, TILE), TILE)

    def build_wide(source, slot):
        def tile(other):
            s = source * plane + lax.rem(p + 2 * plane - 1 - other, plane)
            row, column = tile_row[dom, rep, s], tile_col[dom, rep, s]
            present = row >= 0
            limit = jnp.where(present, tile_count[dom, rep, s], 0)
            row_block = jnp.where(present, row, 0)
            left = across(left_ids[pl.ds(row_block, 1), :])
            right = right_ids[pl.ds(jnp.where(present, column, 0), 1), :]
            bits = bucket(left * (right + 1.0) + 3.0 * right)

            def place(b):
                here = jnp.where(row_block - group_first == b, limit, 0).astype(F32)
                wide[slot, span(b), span(other)] = jnp.where(bits < here, 1.0, 0.0).astype(BF16)

            each(group, place)

        each(plane, tile)

    def build_tall(target):
        s = target * plane + p
        first_own = (s * reps + rep) * own

        def tile(other):
            d = z * plane + lax.rem(p + 2 * plane - 1 - other, plane)
            row, column = tile_row[d, rep, s], tile_col[d, rep, s]
            present = row >= 0
            limit = jnp.where(present, tile_count[d, rep, s], 0)
            left = left_ids[pl.ds(jnp.where(present, row, 0), 1), :]
            right = across(right_ids[pl.ds(jnp.where(present, column, 0), 1), :])
            bits = bucket(left * (right + 1.0) + 3.0 * right)
            for b in range(own):
                here = jnp.where(column - first_own == b, limit, 0).astype(F32)
                tall[target, span(b), span(other)] = jnp.where(bits < here, 1.0, 0.0).astype(BF16)

        each(plane, tile)

    if plan.ahead:
        lax.fori_loop(0, line, lambda i, c: (build_wide(i, i), c)[1], 0)
    lax.fori_loop(0, line, lambda i, c: (build_tall(i), c)[1], 0)

    def count_degrees(s, carry):
        for other in range(reps):
            row, limit = tile_row[dom, other, s], tile_count[dom, other, s]
            carry = tuple(
                value + jnp.where(row == own_first + b, limit, 0) for b, value in enumerate(carry)
            )
        return carry

    degrees = lax.fori_loop(0, plan.doms, count_degrees, (jnp.int32(0),) * own)
    inverse = [
        1.0 / jnp.maximum(jnp.full((8, LANES), degree, jnp.int32).astype(F32), 1.0)[:1]
        for degree in degrees
    ]

    for i in (5, 6, 7):
        loads[i].wait()
    flat_x = x[...].reshape(own * TILE, plan.width_in)
    preact[...] = jnp.dot(flat_x, w_self[...], preferred_element_type=F32)

    def consume(h, slot, source, start):
        for k in range(plane - 1):
            pick_copy(h, slot, k).wait_recv()
        features = picked[h, slot].reshape(plane * TILE, LANES)
        if plan.ahead:
            value = jnp.dot(wide[source], features, preferred_element_type=F32)
            total[h] = value if start else total[h] + value
            return
        build_wide(source, 0)

        def rows(b):
            value = jnp.dot(wide[0, span(b)], features, preferred_element_type=F32)
            total[h, span(b)] = value if start else total[h, span(b)] + value

        each(group, rows)

    def arrive(h, above, k):
        line_copy(h, above, k - 1).wait_recv()

        if k < line - 1:
            @pl.when(passes_on(above))
            def _():
                line_copy(h, above, k).start()

        slot = slot_of(above, k)
        choose(h, slot, spot(above, k), [held[h, slot, b] for b in range(own)])

    def rep_copy(h, peer, slot):
        return remote(
            partial.at[h, peer], landed.at[h, slot], rep_sems, (h, slot), device(z, p, peer)
        )

    def send_partials(h):
        partial[h] = total[h].astype(BF16).reshape(reps, own, TILE, LANES)
        for k, peer in enumerate(rep_peers):
            rep_copy(h, peer, k).start()

    def consume_level(h, k):
        if k == 0:
            consume(h, home, z, True)
            return
        for above, k in levels[k - 1]:
            @pl.when(exists(above, k))
            def _():
                consume(h, slot_of(above, k), spot(above, k), False)

    for k in range(1, line):
        for h in range(halves):
            for above in range(2):
                @pl.when(exists(above, k))
                def _():
                    arrive(h, above, k)
        for h in range(halves):
            consume_level(h, k - 1)
    for h in range(halves):
        consume_level(h, line - 1)
        send_partials(h)

    for h in range(halves):
        for k, peer in enumerate(rep_peers):
            rep_copy(h, peer, k).wait_recv()
        for b in range(own):
            summed = partial[h, rep, b].astype(F32)
            for k in range(reps - 1):
                summed = summed + landed[h, k, b].astype(F32)
            mean[b * TILE : (b + 1) * TILE, half(h)] = (summed * inverse[b]).astype(BF16)
        preact[...] += jnp.dot(
            mean[:, half(h)], w_neigh[half(h), :], preferred_element_type=F32
        )
    value = preact[...]
    logistic = jax.nn.sigmoid(value)
    grad = (cot[...].astype(F32) * logistic * (1.0 + value * (1.0 - logistic))).astype(BF16)

    def spread_copy(h, peer, slot):
        return remote(
            spread[h].at[rep], spread[h].at[rep], spread_sems, (h, slot), device(z, p, peer)
        )

    def spread_arrived(h, k):
        source = lax.rem(rep + reps - k - 1, reps)
        return remote(
            spread[h].at[source], spread[h].at[source], spread_sems, (h, k), device(z, p, source)
        )

    for h in range(halves):
        product = lax.dot_general(grad, w_neigh[half(h), :], OVER_COLS, preferred_element_type=F32)
        for b in range(own):
            spread[h][rep, b] = (product[b * TILE : (b + 1) * TILE] * inverse[b]).astype(BF16)
        for k, peer in enumerate(rep_peers):
            spread_copy(h, peer, k).start()

    both = (x[...].reshape(own * TILE, plan.width_in), mean[...])
    ring_at = col * reps + rep
    ring_peers = []
    for k in range(1, plan.ring):
        other = lax.rem(ring_at + k, plan.ring)
        ring_peers.append(
            (other, device(z, (other // reps) * plan.cores + core, lax.rem(other, reps)))
        )
    core_peers = []
    for k in range(1, plan.cores):
        other = lax.rem(core + k, plan.cores)
        core_peers.append((other, device(z, col * plan.cores + other, rep)))
    far_peers = [(other, device(other, p, rep)) for other in line_peers]

    stages = []
    if plan.split:
        for i, rows in enumerate(both):
            product = lax.dot_general(rows, grad, OVER_ROWS, preferred_element_type=F32)
            terms[i] = product.astype(BF16).reshape(line, plan.ring, plan.strip, plan.width_out)

        def core_copies():
            return [
                remote(terms.at[other], first_in.at[k], core_sems, (k,), to)
                for k, (other, to) in enumerate(core_peers)
            ]

        def far_copies():
            return [
                remote(first.at[other], second_in.at[k], far_sems, (k,), to)
                for k, (other, to) in enumerate(far_peers)
            ]

        def ring_copies():
            return [
                remote(second.at[other], third_in.at[k], ring_sems, (k,), to)
                for k, (other, to) in enumerate(ring_peers)
            ]

        def far_back_copies():
            return [
                remote(final, grads.at[core, z, ring_at], far_back_sems, (k,), to)
                for k, (_, to) in enumerate(far_peers)
            ]

        def ring_back_copies():
            block = grads.at[core, :, ring_at]
            return [
                remote(block, block, ring_back_sems, (k,), to)
                for k, (_, to) in enumerate(ring_peers)
            ]

        def core_back_copies():
            block = grads.at[core]
            return [
                remote(block, block, core_back_sems, (k,), to)
                for k, (_, to) in enumerate(core_peers)
            ]

        def start(copies):
            for copy in copies:
                copy.start()

        def arrived(copies):
            for copy in copies:
                copy.wait_recv()

        def stage_core():
            arrived(core_copies())
            value = terms[core].astype(F32)
            for k in range(len(core_peers)):
                value = value + first_in[k].astype(F32)
            first[...] = value.astype(BF16)
            start(far_copies())

        def stage_far():
            arrived(far_copies())
            value = first[z].astype(F32)
            for k in range(len(far_peers)):
                value = value + second_in[k].astype(F32)
            second[...] = value.astype(BF16)
            start(ring_copies())

        def stage_ring():
            arrived(ring_copies())
            value = second[ring_at].astype(F32)
            for k in range(len(ring_peers)):
                value = value + third_in[k].astype(F32)
            value = (value * scale).astype(BF16)
            final[...] = value
            grads[core, z, ring_at] = value
            start(far_back_copies())

        def stage_ring_back():
            arrived(far_back_copies())
            start(ring_back_copies())

        def stage_core_back():
            arrived(ring_back_copies())
            start(core_back_copies())

        start(core_copies())
        stages = [stage_core, stage_far, stage_ring, stage_ring_back, stage_core_back]
    else:
        for i, rows in enumerate(both):
            grads[i] = lax.dot_general(rows, grad, OVER_ROWS, preferred_element_type=F32)

    def next_stage():
        if stages:
            stages.pop(0)()

    hidden[...] = (value * logistic).astype(BF16)
    back[...] = lax.dot_general(grad, w_self[...], OVER_COLS, preferred_element_type=F32)
    next_stage()

    def pick_back_copy(h, slot, k):
        return remote(
            chosen_back.at[h, slot, k], picked_back.at[h, slot, k], pick_back_sems, (h, slot, k),
            device(z, plane_peers[k], rep),
        )

    def choose_back(h, slot, target):
        def block_for(peer):
            row = tile_row[dom, rep, target * plane + peer]
            offset = jnp.minimum(jnp.maximum(row - group_first, 0), group - 1)
            return spread[h][offset // own, lax.rem(offset, own)]

        for k, peer in enumerate(plane_peers):
            chosen_back[h, slot, k] = block_for(peer)
            pick_back_copy(h, slot, k).start()
        picked_back[h, slot, plane - 1] = block_for(p)

    for h in range(halves):
        for k in range(reps - 1):
            spread_arrived(h, k).wait_recv()
        for above, k in (levels[-1] if levels else []):
            @pl.when(exists(above, k))
            def _():
                choose_back(h, slot_of(above, k), spot(above, k))

    def choose_level(level):
        for above, k in level:
            @pl.when(exists(above, k))
            def _():
                for h in range(halves):
                    choose_back(h, slot_of(above, k), spot(above, k))

    def sum_copy(h, above, k):
        slot = slot_of(above, k)
        nearer = slot_of(above, k - 1) if k > 1 else home
        return remote(
            sums_out.at[h, slot], sums_in.at[above, h, nearer], sum_sems, (above, h, k - 1),
            device(z + 2 * above - 1, p, rep),
        )

    def contribution(h, slot, target):
        for k in range(plane - 1):
            pick_back_copy(h, slot, k).wait_recv()
        return jnp.dot(
            tall[target],
            picked_back[h, slot].reshape(plane * TILE, LANES),
            preferred_element_type=F32,
        )

    def pass_sums(h, above, k):
        slot = slot_of(above, k)
        value = contribution(h, slot, spot(above, k))
        sums_out[h, slot] = value.astype(BF16)
        if k < line - 1:
            @pl.when(passes_on(above))
            def _():
                sum_copy(h, above, k + 1).wait_recv()
                sums_out[h, slot] = (
                    sums_out[h, slot].astype(F32) + sums_in[above, h, slot].astype(F32)
                ).astype(BF16)

        sum_copy(h, above, k).start()

    upper = 2 * z >= line

    def pass_level(level):
        for h in range(halves):
            for above, k, turn in [(1, k, upper) for _, k in level[:1]] + [
                (0, k, None) for _, k in level[:1]
            ] + [(1, k, jnp.logical_not(upper)) for _, k in level[:1]]:
                here = exists(above, k)

                @pl.when(here if turn is None else jnp.logical_and(here, turn))
                def _():
                    pass_sums(h, above, k)

    turn = stages.pop(1) if len(stages) > 1 else None
    for level in reversed(levels[-2:-1]):
        choose_level(level)
    for level in levels[-1:]:
        pass_level(level)
    next_stage()
    for level in reversed(levels[:-2]):
        choose_level(level)
    for h in range(halves):
        choose_back(h, home, z)
    rest = levels[:-1]
    if turn:
        turn()
    for level in rest[-1:]:
        pass_level(level)
    at_end = z * (line - 1 - z) == 0
    turn = stages.pop(0) if stages else None
    if turn:
        @pl.when(jnp.logical_not(at_end))
        def _():
            turn()
    for level in reversed(rest[:-1]):
        pass_level(level)
    if turn:
        @pl.when(at_end)
        def _():
            turn()
    next_stage()
    for h in range(halves):
        back[:, half(h)] += contribution(h, home, z)
        for above in range(2 if line > 1 else 0):
            @pl.when(passes_on(above))
            def _():
                sum_copy(h, above, 1).wait_recv()
                back[:, half(h)] += sums_in[above, h, home].astype(F32)
        feat_grad[:, half(h)] = back[:, half(h)].astype(BF16)
    while stages:
        next_stage()
    if plan.split:
        arrived(core_back_copies())

    for h in range(halves):
        for above in range(2):
            @pl.when(passes_on(above))
            def _():
                line_copy(h, above, 0).wait_send()
            for k in range(1, line):
                if k < line - 1:
                    @pl.when(jnp.logical_and(exists(above, k), passes_on(above)))
                    def _():
                        line_copy(h, above, k).wait_send()

                @pl.when(exists(above, k))
                def _():
                    sum_copy(h, above, k).wait_send()
        for slot in range(line):
            for k in range(plane - 1):
                pick_copy(h, slot, k).wait_send()
                pick_back_copy(h, slot, k).wait_send()
        for k, peer in enumerate(rep_peers):
            rep_copy(h, peer, k).wait_send()
            spread_copy(h, peer, k).wait_send()
    if plan.split:
        for copies in (
            core_copies(), ring_copies(), far_copies(),
            far_back_copies(), ring_back_copies(), core_back_copies(),
        ):
            for copy in copies:
                copy.wait_send()


def write_out(hidden, feat_grad, grads, *refs):
    outs, (wide_grads, sems) = refs[:4], refs[4:]
    copies = [
        pltpu.make_async_copy(src, dst, sems.at[i])
        for i, (src, dst) in enumerate(
            zip((hidden, feat_grad, wide_grads.at[0], wide_grads.at[1]), outs)
        )
    ]
    copies[0].start()
    copies[1].start()
    for i in range(2):
        wide_grads[i] = grads[i].astype(F32).reshape(wide_grads.shape[1:])
        copies[2 + i].start()
    for copy in copies:
        copy.wait()


def dma(*shape):
    return pltpu.SemaphoreType.DMA(tuple(max(size, 1) for size in (2,) + shape))


def shards(
    node_feats, node_ids, tile_row, tile_col, tile_count, self_weight, neigh_weight, out_grad
):
    rows, width_in = node_feats.shape
    width_out = self_weight.shape[1]
    plan = Plan(lax.axis_size("dom"), lax.axis_size("rep"), rows, width_in, width_out)
    line, plane, reps, own, halves = plan.line, plan.plane, plan.reps, plan.own, plan.halves
    scale = 1.0 / math.sqrt(rows * plan.doms * reps)
    id_rows = node_ids.shape[0] // TILE

    def buffer(*shape, dtype=BF16):
        return pltpu.VMEM(tuple(max(size, 1) for size in shape), dtype)

    tile = (TILE, LANES)
    tables = pltpu.SMEM(tile_row.shape, jnp.int32)
    scratch = [
        tables,
        tables,
        tables,
        buffer(id_rows, TILE, dtype=jnp.int32),
        buffer(own, TILE, width_in),
        buffer(rows, width_out),
        buffer(width_in, width_out),
        buffer(width_in, width_out),
        buffer(id_rows, TILE, dtype=F32),
        buffer(id_rows, TILE, dtype=F32),
        buffer(line if plan.ahead else 1, plan.group * TILE, plane * TILE),
        buffer(line, own * TILE, plane * TILE),
        buffer(halves, line, own, *tile),
        buffer(halves, line, plane, *tile),
        buffer(halves, line, plane, *tile),
        buffer(halves, plan.group * TILE, LANES, dtype=F32),
        buffer(halves, reps, own, *tile),
        buffer(halves, reps - 1, own, *tile),
        buffer(rows, width_in),
        buffer(rows, width_out, dtype=F32),
        buffer(rows, width_in, dtype=F32),
        *[buffer(reps, own, *tile) for _ in range(halves)],
        buffer(halves, line, plane, *tile),
        buffer(halves, line, plane, *tile),
        buffer(halves, line, own * TILE, LANES),
        buffer(2, halves, line, own * TILE, LANES),
    ]
    strip = (plan.strip, width_out)
    if plan.split:
        scratch += [
            buffer(plan.cores, line, plan.ring, *strip),
            buffer(plan.cores - 1, line, plan.ring, *strip),
            buffer(line, plan.ring, *strip),
            buffer(line - 1, plan.ring, *strip),
            buffer(plan.ring, *strip),
            buffer(plan.ring - 1, *strip),
            buffer(*strip),
        ]
    scratch += [
        pltpu.SemaphoreType.DMA((8,)),
        dma(2, halves, line),
        dma(halves, line, plane),
        dma(halves, reps - 1),
        dma(halves, reps - 1),
        dma(halves, line, plane),
        dma(2, halves, line),
    ]
    if plan.split:
        scratch += [
            dma(plan.cores - 1), dma(line - 1), dma(plan.ring - 1),
            dma(line - 1), dma(plan.ring - 1), dma(plan.cores - 1),
        ]
        grads_shape = jax.ShapeDtypeStruct((plan.cores, line, plan.ring, *strip), BF16)
    else:
        grads_shape = jax.ShapeDtypeStruct((2, width_in, width_out), F32)
    vmem, anywhere = pl.BlockSpec(memory_space=pltpu.VMEM), pl.BlockSpec(memory_space=pl.ANY)
    hidden_out, feat_grad, grads = pl.pallas_call(
        functools.partial(fused, plan, scale),
        out_shape=(
            pltpu.VMEM((rows, width_out), BF16),
            pltpu.VMEM((rows, width_in), BF16),
            pltpu.VMEM(grads_shape.shape, grads_shape.dtype),
        ),
        in_specs=[anywhere] * 8,
        out_specs=(vmem,) * 3,
        scratch_shapes=scratch,
        compiler_params=pltpu.CompilerParams(collective_id=1, has_side_effects=True),
    )(
        tile_row,
        tile_col,
        tile_count,
        node_ids.reshape(id_rows, TILE),
        node_feats.reshape(own, TILE, width_in),
        out_grad,
        self_weight,
        neigh_weight,
    )
    if not plan.split:
        grads = lax.psum(grads, ("dom", "rep")) * scale
        return hidden_out, feat_grad, grads[0], grads[1]
    grad_shape = jax.ShapeDtypeStruct((width_in, width_out), F32)
    return pl.pallas_call(
        write_out,
        out_shape=(
            jax.ShapeDtypeStruct((rows, width_out), BF16),
            jax.ShapeDtypeStruct((rows, width_in), BF16),
            grad_shape,
            grad_shape,
        ),
        in_specs=[vmem] * 3,
        out_specs=(anywhere,) * 4,
        scratch_shapes=[
            buffer(2, width_in, width_out, dtype=F32),
            pltpu.SemaphoreType.DMA((4,)),
        ],
        compiler_params=pltpu.CompilerParams(vmem_limit_bytes=2**23),
    )(hidden_out, feat_grad, grads)


def solution(mesh):
    placed = (P(("dom", "rep"), None), P(), P(), P(), P(), P(), P(), P(("dom", "rep"), None))
    return jax.shard_map(
        shards,
        mesh=mesh,
        in_specs=placed,
        out_specs=(P(("dom", "rep"), None), P(("dom", "rep"), None), P(), P()),
        check_vma=False,
    )
```

```python
import functools
import math

import jax
import jax.numpy as jnp
from jax import lax
from jax.experimental import pallas as pl
from jax.experimental.pallas import tpu as pltpu
from jax.sharding import PartitionSpec as P

TILE = 128
LANES = 128
HASH = 4099.0

MESH = pl.DeviceIdType.MESH
OVER_ROWS = (((0,), (0,)), ((), ()))
OVER_COLS = (((1,), (1,)), ((), ()))
BF16 = jnp.bfloat16
F32 = jnp.float32


def modulo(value, base):
    quotient = jnp.floor(value * ((1.0 - 2.0**-20) / base))
    left = value - quotient * base
    return jnp.where(left >= base, left - base, left)


def across(row):
    return jnp.broadcast_to(row, (TILE, TILE)).T


def bucket(hashed):
    left = modulo(hashed, HASH)
    return left - jnp.floor(left * (1.0 / TILE)) * TILE


class Plan:
    def __init__(self, dom_total, rep_total, rows, width_in, width_out):
        self.line = math.gcd(dom_total, 4)
        self.plane = dom_total // self.line
        self.cores = math.gcd(self.plane, 2)
        self.cols = self.plane // self.cores
        self.reps = rep_total
        self.doms = dom_total
        self.own = rows // TILE
        self.group = self.own * rep_total
        self.halves = width_in // LANES
        self.width_in, self.width_out = width_in, width_out
        self.ring = self.cols * rep_total
        self.strip = 2 * width_in // (self.cores * self.ring * self.line)
        self.split = self.strip % 16 == 0 and self.cores == 2
        self.ahead = self.line * self.group * self.plane * TILE * TILE * 2 <= 2**23


def fused(plan, scale, *refs):
    refs = list(refs)

    def take(count):
        out, refs[:count] = refs[:count], []
        return out

    line, plane, reps, own, group, halves = (
        plan.line, plan.plane, plan.reps, plan.own, plan.group, plan.halves,
    )
    given = take(8)
    hidden, feat_grad, grads = take(3)
    inputs = take(8)
    tile_row, tile_col, tile_count, ids, x, cot, w_self, w_neigh = inputs
    left_ids, right_ids, wide, tall = take(4)
    held, chosen, picked, total, partial, landed, mean, preact, back = take(9)
    spread = take(halves)
    picked_back, chosen_back, sums_out, sums_in = take(4)
    if plan.split:
        terms, first_in, first, second_in, second, third_in, final = take(7)
    (load_sems,) = take(1)
    line_sems, pick_sems, rep_sems, spread_sems, pick_back_sems, sum_sems = take(6)
    if plan.split:
        core_sems, far_sems, ring_sems, far_back_sems, ring_back_sems, core_back_sems = take(6)

    dom, rep = lax.axis_index("dom"), lax.axis_index("rep")
    z, p = dom // plane, lax.rem(dom, plane)

    def device(zz, pp, rr):
        return (zz * plane + pp, rr)

    def remote(src, dst, sems, index, target):
        return pltpu.make_async_remote_copy(
            src_ref=src,
            dst_ref=dst,
            send_sem=sems.at[(0,) + index],
            recv_sem=sems.at[(1,) + index],
            device_id=target,
            device_id_type=MESH,
        )

    line_peers = [lax.rem(z + k, line) for k in range(1, line)]
    plane_peers = [lax.rem(p + k, plane) for k in range(1, plane)]
    rep_peers = [lax.rem(rep + k, reps) for k in range(1, reps)]
    col, core = p // plan.cores, lax.rem(p, plan.cores)

    everyone = [device(other, p, rep) for other in line_peers]
    everyone += [device(z, other, rep) for other in plane_peers]
    for k in range(plan.cols):
        other = lax.rem(col + k, plan.cols) * plan.cores + core
        everyone += [device(z, other, peer) for peer in rep_peers]
    loads = [
        pltpu.make_async_copy(src, dst, load_sems.at[i])
        for i, (src, dst) in enumerate(zip(given, inputs))
    ]
    for i in (4, 1, 3, 0, 2, 6, 7, 5):
        loads[i].start()
    barrier = pltpu.get_barrier_semaphore()
    for peer in everyone:
        pl.semaphore_signal(barrier, inc=1, device_id=peer, device_id_type=MESH)


    home = line - 1
    levels = [[(above, k) for above in range(2)] for k in range(1, line)]

    def slot_of(above, k):
        return line - 1 - k if above else k - 1

    def spot(above, k):
        return z + k if above else z - k

    def exists(above, k):
        return z < line - k if above else z >= k

    def half(h):
        return slice(h * LANES, (h + 1) * LANES)

    def passes_on(above):
        return z >= 1 if above else z < line - 1

    def line_copy(h, above, k):
        slot = slot_of(above, k + 1)
        src = held.at[h, slot_of(above, k)] if k else x.at[:, :, half(h)]
        return remote(
            src, held.at[h, slot], line_sems, (above, h, k), device(z + 1 - 2 * above, p, rep)
        )

    loads[4].wait()
    pl.semaphore_wait(barrier, len(everyone))

    def choose(h, slot, source, blocks):
        first_own = ((source * plane + p) * reps + rep) * own

        def block_for(d):
            offset = tile_col[d, rep, source * plane + p] - first_own
            value = blocks[0]
            for b in range(1, own):
                value = lax.select(offset == b, blocks[b], value)
            return value

        for k, peer in enumerate(plane_peers):
            chosen[h, slot, k] = block_for(z * plane + peer)
            pick_copy(h, slot, k).start()
        picked[h, slot, plane - 1] = block_for(dom)

    def pick_copy(h, slot, k):
        return remote(
            chosen.at[h, slot, k], picked.at[h, slot, k], pick_sems, (h, slot, k),
            device(z, plane_peers[k], rep),
        )

    for h in range(halves):
        for above in range(2):
            @pl.when(passes_on(above))
            def _():
                line_copy(h, above, 0).start()
    for i in range(4):
        loads[i].wait()
    node = ids[...].astype(F32)
    left_ids[...] = modulo(node, 4093.0)
    right_ids[...] = modulo(node, 4091.0)
    for h in range(halves):
        choose(h, home, z, [x[b, :, half(h)] for b in range(own)])

    group_first = dom * group
    own_first = (dom * reps + rep) * own

    def each(count, body):
        if plan.ahead:
            for i in range(count):
                body(i)
        else:
            lax.fori_loop(0, count, lambda i, c: (body(i), c)[1], 0)

    def span(i):
        return pl.ds(pl.multiple_of(i * TILE, TILE), TILE)

    def build_wide(source, slot):
        def tile(other):
            s = source * plane + lax.rem(p + 2 * plane - 1 - other, plane)
            row, column = tile_row[dom, rep, s], tile_col[dom, rep, s]
            present = row >= 0
            limit = jnp.where(present, tile_count[dom, rep, s], 0)
            row_block = jnp.where(present, row, 0)
            left = across(left_ids[pl.ds(row_block, 1), :])
            right = right_ids[pl.ds(jnp.where(present, column, 0), 1), :]
            bits = bucket(left * (right + 1.0) + 3.0 * right)

            def place(b):
                here = jnp.where(row_block - group_first == b, limit, 0).astype(F32)
                wide[slot, span(b), span(other)] = jnp.where(bits < here, 1.0, 0.0).astype(BF16)

            each(group, place)

        each(plane, tile)

    def build_tall(target):
        s = target * plane + p
        first_own = (s * reps + rep) * own

        def tile(other):
            d = z * plane + lax.rem(p + 2 * plane - 1 - other, plane)
            row, column = tile_row[d, rep, s], tile_col[d, rep, s]
            present = row >= 0
            limit = jnp.where(present, tile_count[d, rep, s], 0)
            left = left_ids[pl.ds(jnp.where(present, row, 0), 1), :]
            right = across(right_ids[pl.ds(jnp.where(present, column, 0), 1), :])
            bits = bucket(left * (right + 1.0) + 3.0 * right)
            for b in range(own):
                here = jnp.where(column - first_own == b, limit, 0).astype(F32)
                tall[target, span(b), span(other)] = jnp.where(bits < here, 1.0, 0.0).astype(BF16)

        each(plane, tile)

    if plan.ahead:
        lax.fori_loop(0, line, lambda i, c: (build_wide(i, i), c)[1], 0)
    lax.fori_loop(0, line, lambda i, c: (build_tall(i), c)[1], 0)

    def count_degrees(s, carry):
        for other in range(reps):
            row, limit = tile_row[dom, other, s], tile_count[dom, other, s]
            carry = tuple(
                value + jnp.where(row == own_first + b, limit, 0) for b, value in enumerate(carry)
            )
        return carry

    degrees = lax.fori_loop(0, plan.doms, count_degrees, (jnp.int32(0),) * own)
    inverse = [
        1.0 / jnp.maximum(jnp.full((8, LANES), degree, jnp.int32).astype(F32), 1.0)[:1]
        for degree in degrees
    ]

    for i in (5, 6, 7):
        loads[i].wait()
    flat_x = x[...].reshape(own * TILE, plan.width_in)
    preact[...] = jnp.dot(flat_x, w_self[...], preferred_element_type=F32)

    def consume(h, slot, source, start):
        for k in range(plane - 1):
            pick_copy(h, slot, k).wait_recv()
        features = picked[h, slot].reshape(plane * TILE, LANES)
        if plan.ahead:
            value = jnp.dot(wide[source], features, preferred_element_type=F32)
            total[h] = value if start else total[h] + value
            return
        build_wide(source, 0)

        def rows(b):
            value = jnp.dot(wide[0, span(b)], features, preferred_element_type=F32)
            total[h, span(b)] = value if start else total[h, span(b)] + value

        each(group, rows)

    def arrive(h, above, k):
        line_copy(h, above, k - 1).wait_recv()

        if k < line - 1:
            @pl.when(passes_on(above))
            def _():
                line_copy(h, above, k).start()

        slot = slot_of(above, k)
        choose(h, slot, spot(above, k), [held[h, slot, b] for b in range(own)])

    def rep_copy(h, peer, slot):
        return remote(
            partial.at[h, peer], landed.at[h, slot], rep_sems, (h, slot), device(z, p, peer)
        )

    def send_partials(h):
        partial[h] = total[h].astype(BF16).reshape(reps, own, TILE, LANES)
        for k, peer in enumerate(rep_peers):
            rep_copy(h, peer, k).start()

    def consume_level(h, k):
        if k == 0:
            consume(h, home, z, True)
            return
        for above, k in levels[k - 1]:
            @pl.when(exists(above, k))
            def _():
                consume(h, slot_of(above, k), spot(above, k), False)

    for k in range(1, line):
        for h in range(halves):
            for above in range(2):
                @pl.when(exists(above, k))
                def _():
                    arrive(h, above, k)
        for h in range(halves):
            consume_level(h, k - 1)
    for h in range(halves):
        consume_level(h, line - 1)
        send_partials(h)

    for h in range(halves):
        for k, peer in enumerate(rep_peers):
            rep_copy(h, peer, k).wait_recv()
        for b in range(own):
            summed = partial[h, rep, b].astype(F32)
            for k in range(reps - 1):
                summed = summed + landed[h, k, b].astype(F32)
            mean[b * TILE : (b + 1) * TILE, half(h)] = (summed * inverse[b]).astype(BF16)
        preact[...] += jnp.dot(
            mean[:, half(h)], w_neigh[half(h), :], preferred_element_type=F32
        )
    value = preact[...]
    logistic = jax.nn.sigmoid(value)
    grad = (cot[...].astype(F32) * logistic * (1.0 + value * (1.0 - logistic))).astype(BF16)

    def spread_copy(h, peer, slot):
        return remote(
            spread[h].at[rep], spread[h].at[rep], spread_sems, (h, slot), device(z, p, peer)
        )

    def spread_arrived(h, k):
        source = lax.rem(rep + reps - k - 1, reps)
        return remote(
            spread[h].at[source], spread[h].at[source], spread_sems, (h, k), device(z, p, source)
        )

    def spread_half(h):
        product = lax.dot_general(grad, w_neigh[half(h), :], OVER_COLS, preferred_element_type=F32)
        for b in range(own):
            spread[h][rep, b] = (product[b * TILE : (b + 1) * TILE] * inverse[b]).astype(BF16)
        for k, peer in enumerate(rep_peers):
            spread_copy(h, peer, k).start()

    spread_half(0)
    both = (x[...].reshape(own * TILE, plan.width_in), mean[...])
    ring_at = col * reps + rep
    ring_peers = []
    for k in range(1, plan.ring):
        other = lax.rem(ring_at + k, plan.ring)
        ring_peers.append(
            (other, device(z, (other // reps) * plan.cores + core, lax.rem(other, reps)))
        )
    core_peers = []
    for k in range(1, plan.cores):
        other = lax.rem(core + k, plan.cores)
        core_peers.append((other, device(z, col * plan.cores + other, rep)))
    far_peers = [(other, device(other, p, rep)) for other in line_peers]

    stages = []
    if plan.split:
        for i, rows in enumerate(both):
            product = lax.dot_general(rows, grad, OVER_ROWS, preferred_element_type=F32)
            terms[i] = product.astype(BF16).reshape(line, plan.ring, plan.strip, plan.width_out)

        def core_copies():
            return [
                remote(terms.at[other], first_in.at[k], core_sems, (k,), to)
                for k, (other, to) in enumerate(core_peers)
            ]

        def far_copies():
            return [
                remote(first.at[other], second_in.at[k], far_sems, (k,), to)
                for k, (other, to) in enumerate(far_peers)
            ]

        def ring_copies():
            return [
                remote(second.at[other], third_in.at[k], ring_sems, (k,), to)
                for k, (other, to) in enumerate(ring_peers)
            ]

        def far_back_copies():
            return [
                remote(final, grads.at[core, z, ring_at], far_back_sems, (k,), to)
                for k, (_, to) in enumerate(far_peers)
            ]

        def ring_back_copies():
            block = grads.at[core, :, ring_at]
            return [
                remote(block, block, ring_back_sems, (k,), to)
                for k, (_, to) in enumerate(ring_peers)
            ]

        def core_back_copies():
            block = grads.at[core]
            return [
                remote(block, block, core_back_sems, (k,), to)
                for k, (_, to) in enumerate(core_peers)
            ]

        def start(copies):
            for copy in copies:
                copy.start()

        def arrived(copies):
            for copy in copies:
                copy.wait_recv()

        def stage_core():
            arrived(core_copies())
            value = terms[core].astype(F32)
            for k in range(len(core_peers)):
                value = value + first_in[k].astype(F32)
            first[...] = value.astype(BF16)
            start(far_copies())

        def stage_far():
            arrived(far_copies())
            value = first[z].astype(F32)
            for k in range(len(far_peers)):
                value = value + second_in[k].astype(F32)
            second[...] = value.astype(BF16)
            start(ring_copies())

        def stage_ring():
            arrived(ring_copies())
            value = second[ring_at].astype(F32)
            for k in range(len(ring_peers)):
                value = value + third_in[k].astype(F32)
            value = (value * scale).astype(BF16)
            final[...] = value
            grads[core, z, ring_at] = value
            start(far_back_copies())

        def stage_ring_back():
            arrived(far_back_copies())
            start(ring_back_copies())

        def stage_core_back():
            arrived(ring_back_copies())
            start(core_back_copies())

        start(core_copies())
        stages = [stage_core, stage_far, stage_ring, stage_ring_back, stage_core_back]
    else:
        for i, rows in enumerate(both):
            grads[i] = lax.dot_general(rows, grad, OVER_ROWS, preferred_element_type=F32)

    def next_stage():
        if stages:
            stages.pop(0)()

    for h in range(1, halves):
        spread_half(h)
    hidden[...] = (value * logistic).astype(BF16)
    next_stage()
    back[...] = lax.dot_general(grad, w_self[...], OVER_COLS, preferred_element_type=F32)

    def pick_back_copy(h, slot, k):
        return remote(
            chosen_back.at[h, slot, k], picked_back.at[h, slot, k], pick_back_sems, (h, slot, k),
            device(z, plane_peers[k], rep),
        )

    def choose_back(h, slot, target):
        def block_for(peer):
            row = tile_row[dom, rep, target * plane + peer]
            offset = jnp.minimum(jnp.maximum(row - group_first, 0), group - 1)
            return spread[h][offset // own, lax.rem(offset, own)]

        for k, peer in enumerate(plane_peers):
            chosen_back[h, slot, k] = block_for(peer)
            pick_back_copy(h, slot, k).start()
        picked_back[h, slot, plane - 1] = block_for(p)

    for h in range(halves):
        for k in range(reps - 1):
            spread_arrived(h, k).wait_recv()
        for above, k in (levels[-1] if levels else []):
            @pl.when(exists(above, k))
            def _():
                choose_back(h, slot_of(above, k), spot(above, k))

    def choose_level(level):
        for above, k in level:
            @pl.when(exists(above, k))
            def _():
                for h in range(halves):
                    choose_back(h, slot_of(above, k), spot(above, k))

    def sum_copy(h, above, k):
        slot = slot_of(above, k)
        nearer = slot_of(above, k - 1) if k > 1 else home
        return remote(
            sums_out.at[h, slot], sums_in.at[above, h, nearer], sum_sems, (above, h, k - 1),
            device(z + 2 * above - 1, p, rep),
        )

    def contribution(h, slot, target):
        for k in range(plane - 1):
            pick_back_copy(h, slot, k).wait_recv()
        return jnp.dot(
            tall[target],
            picked_back[h, slot].reshape(plane * TILE, LANES),
            preferred_element_type=F32,
        )

    def pass_sums(h, above, k):
        slot = slot_of(above, k)
        value = contribution(h, slot, spot(above, k))
        sums_out[h, slot] = value.astype(BF16)
        if k < line - 1:
            @pl.when(passes_on(above))
            def _():
                sum_copy(h, above, k + 1).wait_recv()
                sums_out[h, slot] = (
                    sums_out[h, slot].astype(F32) + sums_in[above, h, slot].astype(F32)
                ).astype(BF16)

        sum_copy(h, above, k).start()

    upper = 2 * z >= line

    def pass_level(level):
        for h in range(halves):
            for above, k, turn in [(1, k, upper) for _, k in level[:1]] + [
                (0, k, None) for _, k in level[:1]
            ] + [(1, k, jnp.logical_not(upper)) for _, k in level[:1]]:
                here = exists(above, k)

                @pl.when(here if turn is None else jnp.logical_and(here, turn))
                def _():
                    pass_sums(h, above, k)

    turn = stages.pop(1) if len(stages) > 1 else None
    for level in reversed(levels[-2:-1]):
        choose_level(level)
    for level in levels[-1:]:
        pass_level(level)
    next_stage()
    for level in reversed(levels[:-2]):
        choose_level(level)
    for h in range(halves):
        choose_back(h, home, z)
    rest = levels[:-1]
    if turn:
        turn()
    for level in rest[-1:]:
        pass_level(level)
    at_end = z * (line - 1 - z) == 0
    turn = stages.pop(0) if stages else None
    if turn:
        @pl.when(jnp.logical_not(at_end))
        def _():
            turn()
    for level in reversed(rest[:-1]):
        pass_level(level)
    if turn:
        @pl.when(at_end)
        def _():
            turn()
    next_stage()
    for h in range(halves):
        back[:, half(h)] += contribution(h, home, z)
        for above in range(2 if line > 1 else 0):
            @pl.when(passes_on(above))
            def _():
                sum_copy(h, above, 1).wait_recv()
                back[:, half(h)] += sums_in[above, h, home].astype(F32)
        feat_grad[:, half(h)] = back[:, half(h)].astype(BF16)
    while stages:
        next_stage()
    if plan.split:
        arrived(core_back_copies())

    for h in range(halves):
        for above in range(2):
            @pl.when(passes_on(above))
            def _():
                line_copy(h, above, 0).wait_send()
            for k in range(1, line):
                if k < line - 1:
                    @pl.when(jnp.logical_and(exists(above, k), passes_on(above)))
                    def _():
                        line_copy(h, above, k).wait_send()

                @pl.when(exists(above, k))
                def _():
                    sum_copy(h, above, k).wait_send()
        for slot in range(line):
            for k in range(plane - 1):
                pick_copy(h, slot, k).wait_send()
                pick_back_copy(h, slot, k).wait_send()
        for k, peer in enumerate(rep_peers):
            rep_copy(h, peer, k).wait_send()
            spread_copy(h, peer, k).wait_send()
    if plan.split:
        for copies in (
            core_copies(), ring_copies(), far_copies(),
            far_back_copies(), ring_back_copies(), core_back_copies(),
        ):
            for copy in copies:
                copy.wait_send()


def write_out(hidden, feat_grad, grads, *refs):
    outs, (wide_grads, sems) = refs[:4], refs[4:]
    copies = [
        pltpu.make_async_copy(src, dst, sems.at[i])
        for i, (src, dst) in enumerate(
            zip((hidden, feat_grad, wide_grads.at[0], wide_grads.at[1]), outs)
        )
    ]
    copies[0].start()
    copies[1].start()
    for i in range(2):
        wide_grads[i] = grads[i].astype(F32).reshape(wide_grads.shape[1:])
        copies[2 + i].start()
    for copy in copies:
        copy.wait()


def dma(*shape):
    return pltpu.SemaphoreType.DMA(tuple(max(size, 1) for size in (2,) + shape))


def shards(
    node_feats, node_ids, tile_row, tile_col, tile_count, self_weight, neigh_weight, out_grad
):
    rows, width_in = node_feats.shape
    width_out = self_weight.shape[1]
    plan = Plan(lax.axis_size("dom"), lax.axis_size("rep"), rows, width_in, width_out)
    line, plane, reps, own, halves = plan.line, plan.plane, plan.reps, plan.own, plan.halves
    scale = 1.0 / math.sqrt(rows * plan.doms * reps)
    id_rows = node_ids.shape[0] // TILE

    def buffer(*shape, dtype=BF16):
        return pltpu.VMEM(tuple(max(size, 1) for size in shape), dtype)

    tile = (TILE, LANES)
    tables = pltpu.SMEM(tile_row.shape, jnp.int32)
    scratch = [
        tables,
        tables,
        tables,
        buffer(id_rows, TILE, dtype=jnp.int32),
        buffer(own, TILE, width_in),
        buffer(rows, width_out),
        buffer(width_in, width_out),
        buffer(width_in, width_out),
        buffer(id_rows, TILE, dtype=F32),
        buffer(id_rows, TILE, dtype=F32),
        buffer(line if plan.ahead else 1, plan.group * TILE, plane * TILE),
        buffer(line, own * TILE, plane * TILE),
        buffer(halves, line, own, *tile),
        buffer(halves, line, plane, *tile),
        buffer(halves, line, plane, *tile),
        buffer(halves, plan.group * TILE, LANES, dtype=F32),
        buffer(halves, reps, own, *tile),
        buffer(halves, reps - 1, own, *tile),
        buffer(rows, width_in),
        buffer(rows, width_out, dtype=F32),
        buffer(rows, width_in, dtype=F32),
        *[buffer(reps, own, *tile) for _ in range(halves)],
        buffer(halves, line, plane, *tile),
        buffer(halves, line, plane, *tile),
        buffer(halves, line, own * TILE, LANES),
        buffer(2, halves, line, own * TILE, LANES),
    ]
    strip = (plan.strip, width_out)
    if plan.split:
        scratch += [
            buffer(plan.cores, line, plan.ring, *strip),
            buffer(plan.cores - 1, line, plan.ring, *strip),
            buffer(line, plan.ring, *strip),
            buffer(line - 1, plan.ring, *strip),
            buffer(plan.ring, *strip),
            buffer(plan.ring - 1, *strip),
            buffer(*strip),
        ]
    scratch += [
        pltpu.SemaphoreType.DMA((8,)),
        dma(2, halves, line),
        dma(halves, line, plane),
        dma(halves, reps - 1),
        dma(halves, reps - 1),
        dma(halves, line, plane),
        dma(2, halves, line),
    ]
    if plan.split:
        scratch += [
            dma(plan.cores - 1), dma(line - 1), dma(plan.ring - 1),
            dma(line - 1), dma(plan.ring - 1), dma(plan.cores - 1),
        ]
        grads_shape = jax.ShapeDtypeStruct((plan.cores, line, plan.ring, *strip), BF16)
    else:
        grads_shape = jax.ShapeDtypeStruct((2, width_in, width_out), F32)
    vmem, anywhere = pl.BlockSpec(memory_space=pltpu.VMEM), pl.BlockSpec(memory_space=pl.ANY)
    hidden_out, feat_grad, grads = pl.pallas_call(
        functools.partial(fused, plan, scale),
        out_shape=(
            pltpu.VMEM((rows, width_out), BF16),
            pltpu.VMEM((rows, width_in), BF16),
            pltpu.VMEM(grads_shape.shape, grads_shape.dtype),
        ),
        in_specs=[anywhere] * 8,
        out_specs=(vmem,) * 3,
        scratch_shapes=scratch,
        compiler_params=pltpu.CompilerParams(collective_id=1, has_side_effects=True),
    )(
        tile_row,
        tile_col,
        tile_count,
        node_ids.reshape(id_rows, TILE),
        node_feats.reshape(own, TILE, width_in),
        out_grad,
        self_weight,
        neigh_weight,
    )
    if not plan.split:
        grads = lax.psum(grads, ("dom", "rep")) * scale
        return hidden_out, feat_grad, grads[0], grads[1]
    grad_shape = jax.ShapeDtypeStruct((width_in, width_out), F32)
    return pl.pallas_call(
        write_out,
        out_shape=(
            jax.ShapeDtypeStruct((rows, width_out), BF16),
            jax.ShapeDtypeStruct((rows, width_in), BF16),
            grad_shape,
            grad_shape,
        ),
        in_specs=[vmem] * 3,
        out_specs=(anywhere,) * 4,
        scratch_shapes=[
            buffer(2, width_in, width_out, dtype=F32),
            pltpu.SemaphoreType.DMA((4,)),
        ],
        compiler_params=pltpu.CompilerParams(vmem_limit_bytes=2**23),
    )(hidden_out, feat_grad, grads)


def solution(mesh):
    placed = (P(("dom", "rep"), None), P(), P(), P(), P(), P(), P(), P(("dom", "rep"), None))
    return jax.shard_map(
        shards,
        mesh=mesh,
        in_specs=placed,
        out_specs=(P(("dom", "rep"), None), P(("dom", "rep"), None), P(), P()),
        check_vma=False,
    )
```
